128 devices in a mesh: gz: 128 (over x, y, z, core).
Axes of the slice: x: 4, y: 4, z: 4, core: 2. Of those that a mesh axis runs over, the one named last changes fastest.
Arguments:
- velocity: float32 [3, 512, 256, 512], P(None, 'gz'), may hold values from -0.3 to 0.3
- offsets: float32 [3, 65536], P(None, 'gz'), may hold values from 1.2 to 1.8
- bases: int32 [3, 65536], P(None, 'gz'), may hold values from 0 to 511, as said below
- targets: float32 [3, 65536], P(None, 'gz'), may hold values from 1 to 2
- stiffness: float32 [65536], P('gz'), may hold values from 10 to 100
- active_block_count: int32 [128], P('gz'), may hold values from 1 to 2, as said below
Outputs:
- velocity_out: float32 [3, 512, 256, 512], P(None, 'gz')
- offsets_out: float32 [3, 65536], P(None, 'gz')
The draws below stay inside these ranges and needn't reach their ends.
Inputs may be any that keep to these rules, and one draw needn't show every extreme that they name: `bases`: rows are x, y, z. x lies in 0..511 and y in 0..255; the z of marker m lies in the slab of index m // 512, from (m // 512) * 4 to (m // 512) * 4 + 3. `active_block_count`: in every draw some slab uses all 2 blocks.
All inputs are finite; a program needn't handle non-finite values.
Results may differ from the reference program's by a relative error of at most 0.0015.
Values may be sent and summed in bfloat16 or wider, within the bound.
A program may use at most 192 MiB of HBM per device.

```python
import math
import jax
import jax.numpy as jnp
from jax import lax

NX = 512
NY = 256
CZ = 4
M_DEV = 512
BLK = 256
STEPS = 2
NBLK = 2
NZ = 512
MARKERS = 65536
SLABS = 128


def draw_bases(key, part):
    first_key, second_key, third_key = jax.random.split(key, 3)
    x_cells = jax.random.randint(first_key, (MARKERS,), 0, NX)
    y_cells = jax.random.randint(second_key, (MARKERS,), 0, NY)
    owners = jnp.arange(MARKERS, dtype=jnp.int32) // M_DEV
    z_cells = owners * CZ + jax.random.randint(third_key, (MARKERS,), 0, CZ)
    return jnp.stack([x_cells, y_cells, z_cells]).astype(jnp.int32)


def draw_active_block_count(key, part):
    count_key, chosen_key = jax.random.split(key)
    counts = jax.random.randint(count_key, (SLABS,), 1, NBLK + 1)
    chosen = jax.random.randint(chosen_key, (), 0, SLABS)
    return counts.at[chosen].set(NBLK).astype(jnp.int32)


def block_levels(own_key, extent, cuts, low, largest):
    def one(dim, parts):
        heights = jax.random.uniform(jax.random.fold_in(jax.random.fold_in(own_key, 6), dim), (parts,), jnp.float32, low / len(cuts), largest / len(cuts))
        return jnp.repeat(jnp.exp(heights), extent[dim] // parts).reshape((-1,) + (1,) * (len(extent) - dim - 1))

    level = one(*cuts[0])
    for cut in cuts[1:]:
        level = level * one(*cut)
    return level


def bell_draw(own_key, extent, width, bound, pieces=(), held_as=jnp.bfloat16):
    drawn = jax.random.normal(own_key, extent, jnp.float32) * width
    if len(pieces) > 0:
        drawn = block_levels(own_key, extent, pieces, -0.22, 0.18) * drawn
    return jnp.clip(drawn, min=-bound, max=bound).astype(held_as)


def setup_inputs(seed: int = 0) -> dict:
    keys = jax.random.split(jax.random.key(seed), 7)
    return {
        "velocity": bell_draw(keys[0], (3, NZ, NY, NX), 0.1, 0.3, ((1, 128),), jnp.float32),
        "offsets": jnp.clip(1.2 + 0.5999999 * jax.random.uniform(keys[1], (3, MARKERS), jnp.float32) ** block_levels(keys[1], (3, MARKERS), ((1, 128),), -0.2, 0.2), 1.2, 1.8),
        "bases": draw_bases(jax.random.fold_in(keys[6], 71), 0),
        "targets": jnp.clip(1.0 + 1.0 * jax.random.uniform(keys[3], (3, MARKERS), jnp.float32) ** block_levels(keys[3], (3, MARKERS), ((1, 128),), -0.2, 0.2), 1.0, 2.0),
        "stiffness": jnp.clip(jnp.exp(math.log(100.0) - 2.3025851 * jax.random.uniform(keys[4], (MARKERS,), jnp.float32) ** block_levels(keys[4], (MARKERS,), ((0, 128),), -0.2, 0.2)), 10.0, 100.0),
        "active_block_count": draw_active_block_count(jax.random.fold_in(keys[6], 71), 0),
    }


def kernel(offsets):
    steps_back = jnp.arange(4).astype(jnp.float32)
    return 0.25 * (1.0 + jnp.cos((0.5 * math.pi) * (offsets[:, None, :] - steps_back[None, :, None])))


def advance(velocity, forcing):
    laplace = -6.0 * velocity
    transport_velocity = jnp.zeros_like(velocity)
    for sweep_sense in (1, 2, 3):
        upper_cells = jnp.roll(velocity, -1, sweep_sense)
        lower_cells = jnp.roll(velocity, 1, sweep_sense)
        transfer_buffer = 3 - sweep_sense
        laplace = laplace + upper_cells + lower_cells
        transport_velocity = transport_velocity + velocity[transfer_buffer][None] * (upper_cells - lower_cells) * 0.5
    return velocity + 0.2 * (0.3 * laplace - transport_velocity + forcing)


def rounded(values):
    return lax.optimization_barrier(values.astype(jnp.bfloat16)).astype(jnp.float32)


def reference(velocity, offsets, bases, targets, stiffness, active_block_count):
    markers = offsets.shape[1]
    ordinal = jnp.arange(markers, dtype=jnp.int32)
    living = ((ordinal % M_DEV) // BLK < active_block_count[ordinal // M_DEV]).astype(jnp.float32)
    reach = jnp.arange(4, dtype=jnp.int32)
    xcells = (bases[0][None, :] + reach[:, None]) % NX
    ycells = (bases[1][None, :] + reach[:, None]) % NY
    zcells = (bases[2][None, :] + reach[:, None]) % NZ
    shape_all = (4, 4, 4, markers)
    z_index = jnp.broadcast_to(zcells[:, None, None, :], shape_all).reshape(-1)
    y_index = jnp.broadcast_to(ycells[None, :, None, :], shape_all).reshape(-1)
    x_index = jnp.broadcast_to(xcells[None, None, :, :], shape_all).reshape(-1)
    for step_number in range(STEPS):
        weights = kernel(offsets)
        forces = living[None, :] * stiffness[None, :] * (targets - offsets)
        vertical = rounded((forces[:, None, None, :] * weights[2][None, :, None, :]) * weights[1][None, None, :, :])
        across = rounded(weights[0])
        amounts = vertical[:, :, :, None, :] * across[None, None, None, :, :]
        forcing = jnp.zeros_like(velocity).at[:, z_index, y_index, x_index].add(amounts.reshape(3, -1))
        velocity = advance(velocity, forcing)
        lowered = velocity.astype(jnp.bfloat16)
        picked = lowered[:, z_index, y_index, x_index].astype(jnp.float32).reshape(3, 4, 4, 4, markers)
        mixed = rounded(weights[2][:, None, :] * weights[1][None, :, :])
        sampled = jnp.sum((mixed[None, :, :, None, :] * picked) * weights[0][None, None, None, :, :], axis=(1, 2, 3))
        offsets = offsets + 0.2 * (living[None, :] * sampled)
    return velocity, offsets
```

```python
import functools
import math

import jax
import jax.numpy as jnp
from jax import lax
from jax.experimental import pallas as pl
from jax.experimental.pallas import tpu as pltpu
from jax.sharding import PartitionSpec as P

AXIS = "gz"
BLK = 256
STEPS = 2
DT = 0.2
NU = 0.3
CZ = 4
NY = 256
NX = 512
M = 512
MESH = pl.DeviceIdType.MESH
BF = jnp.bfloat16
F32 = jnp.float32


def weights(offsets):
    angle = offsets * (0.5 * math.pi)
    c = 0.25 * jnp.cos(angle)
    s = 0.25 * jnp.sin(angle)
    return (0.25 + c, 0.25 + s, 0.25 - c, 0.25 - s)


def pick(delta, taps):
    out = jnp.where(delta == 3, taps[3], 0.0)
    for j in (2, 1, 0):
        out = jnp.where(delta == j, taps[j], out)
    return out


def kernel(
    vel, off_ref, bases_ref, targ_ref, stiff_ref, act_ref,
    vout, oout,
    state, low, edge, halo, xtab, ytab, lhs, gains, zrows, pack, near, ret, back, offs,
    in_sem, out_sem, send_sem, recv_sem, psend, precv, rsend, rrecv,
):
    me = lax.axis_index(AXIS)
    count = lax.axis_size(AXIS)
    right = lax.rem(me + 1, count)
    left = lax.rem(me + count - 1, count)

    loads = {}
    for p in (0, 3, 1, 2):
        loads[p] = pltpu.make_async_copy(vel.at[:, p], state.at[0, p], in_sem.at[p])
        loads[p].start()

    barrier = pltpu.get_barrier_semaphore()
    for neighbour in (left, right):
        pl.semaphore_signal(barrier, inc=1, device_id=(neighbour,), device_id_type=MESH)

    lane = lax.broadcasted_iota(jnp.int32, (1, M), 1)
    living = jnp.where(lane < act_ref[...] * BLK, 1.0, 0.0)
    strength = living * stiff_ref[...]
    level = bases_ref[2:3, :] - me * CZ
    offs[...] = off_ref[...]

    def prepare(slot):
        o = offs[...]
        w = weights(o)
        force = strength * (targ_ref[...] - o)
        for j in range(4):
            pack[slot, 6 + j : 7 + j, :] = w[j][0:1]
            pack[slot, 10 + j : 11 + j, :] = w[j][1:2]
        pack[slot, 0:3, :] = force
        pack[slot, 14:16, :] = bases_ref[0:2, :].astype(F32)
        for z in range(7):
            row = pick(z - level, [w[j][2:3] for j in range(4)])
            if z < CZ:
                zrows[z, 0:1, 0:M] = row
                gains[z, 0:3, 0:M] = force * row
            else:
                pack[slot, 3 + z - CZ : 4 + z - CZ, :] = row

    def receive(slot):
        zrows[CZ - 1, 0:1, M:] = jnp.zeros((1, M), F32)
        for z in range(3):
            row = near[slot, 3 + z : 4 + z, :]
            zrows[z, 0:1, M:] = row
            gains[z, 0:3, M:] = near[slot, 0:3, :] * row

    def tables(source, slot, side):
        lanes = pl.ds(side * M, M)

        def xrow(i, _):
            r = pl.multiple_of(i * 16, 16)
            where = lax.broadcasted_iota(jnp.int32, (16, M), 0) + r
            delta = (where - source[slot, 14:15, :].astype(jnp.int32)) & (NX - 1)
            taps = [source[slot, 6 + j : 7 + j, :] for j in range(4)]
            xtab[pl.ds(r, 16), lanes] = pick(delta, taps).astype(BF)
            return 0

        lax.fori_loop(0, NX // 16, xrow, 0)

        def yrow(i, _):
            r = pl.multiple_of(i * 16, 16)
            where = lax.broadcasted_iota(jnp.int32, (16, M), 0) + r
            delta = (where - source[slot, 15:16, :].astype(jnp.int32)) & (NY - 1)
            taps = [source[slot, 10 + j : 11 + j, :] for j in range(4)]
            ytab[pl.ds(r, 16), lanes] = pick(delta, taps)
            return 0

        lax.fori_loop(0, NY // 16, yrow, 0)

    def spread(z, width, dst):
        def rows(i, _):
            r = pl.multiple_of(i * 16, 16)
            y = ytab[pl.ds(r, 16), 0:width]
            for c in range(3):
                lhs[pl.ds(c * NY + r, 16), 0:width] = (gains[z, c : c + 1, 0:width] * y).astype(BF)
            return 0

        lax.fori_loop(0, NY // 16, rows, 0)
        out = lax.dot_general(
            lhs[:, 0:width],
            xtab[:, 0:width],
            (((1,), (1,)), ((), ())),
            preferred_element_type=F32,
        )
        state[dst, z] = out.reshape(3, NY, NX)

    def spread_all(dst):
        def body(z, _):
            spread(z, 2 * M, dst)
            return 0

        lax.fori_loop(0, CZ - 1, body, 0)
        spread(CZ - 1, M, dst)

    def advance(p, src, dst, below, above):
        def rows(i, _):
            r = pl.multiple_of(i * 16, 16)
            rp = pl.multiple_of(lax.rem(r + NY - 8, NY), 8)
            rn = pl.multiple_of(lax.rem(r + 16, NY), 8)
            here = pl.ds(r, 16)
            v = [state[src, p, c, here, :] for c in range(3)]
            lower, upper = [], []
            for d in (2, 1, 0):
                scaled = (0.5 * DT) * v[d]
                upper.append(DT * NU - scaled)
                lower.append(DT * NU + scaled)
            for c in range(3):
                prev = state[src, p, c, pl.ds(rp, 8), :]
                nxt = state[src, p, c, pl.ds(rn, 8), :]
                total = DT * state[dst, p, c, here, :] + (1.0 - 6.0 * DT * NU) * v[c]
                total = total + upper[0] * above(c, here) + lower[0] * below(c, here)
                yup = pltpu.roll(jnp.concatenate([v[c], nxt], axis=0), 23, 0)[0:16]
                ydown = pltpu.roll(jnp.concatenate([prev, v[c]], axis=0), 1, 0)[8:24]
                total = total + upper[1] * yup + lower[1] * ydown
                total = total + upper[2] * pltpu.roll(v[c], NX - 1, 1) + lower[2] * pltpu.roll(v[c], 1, 1)
                state[dst, p, c, here, :] = total
                low[p, c, here, :] = total.astype(BF)
            return 0

        lax.fori_loop(0, NY // 16, rows, 0)

    def inner(src, plane):
        return lambda c, rows: state[src, plane, c, rows, :]

    def outer(step, side):
        return lambda c, rows: halo[step, side, c, rows, :].astype(F32)

    def sample(z, lanes):
        out = jnp.dot(low[z].reshape(3 * NY, NX), xtab[:, lanes], preferred_element_type=F32)
        y = ytab[:, lanes]
        parts = [jnp.sum(out[c * NY : (c + 1) * NY] * y, axis=0, keepdims=True) for c in range(3)]
        return jnp.concatenate(parts, axis=0) * zrows[z, 0:1, lanes]

    own = slice(0, M)
    other = slice(M, 2 * M)

    waits = []
    for step in range(STEPS):
        src, dst = step % 2, (step + 1) % 2
        prepare(step)
        if step == 0:
            for side, p in ((0, 0), (1, 3)):
                loads[p].wait()

                def lower_rows(i, _, side=side, p=p):
                    r = pl.multiple_of(i * 16, 16)
                    for c in range(3):
                        edge[side, c, pl.ds(r, 16), :] = state[0, p, c, pl.ds(r, 16), :].astype(BF)
                    return 0

                lax.fori_loop(0, NY // 16, lower_rows, 0)
            pl.semaphore_wait(barrier, 2)
        packet = pltpu.make_async_remote_copy(
            src_ref=pack.at[step], dst_ref=near.at[step],
            send_sem=psend.at[step], recv_sem=precv.at[step],
            device_id=(right,), device_id_type=MESH,
        )
        packet.start()
        if step == 0:
            copies = []
            for side, target in ((0, left), (1, right)):
                copies.append(pltpu.make_async_remote_copy(
                    src_ref=edge.at[side], dst_ref=halo.at[0, 1 - side],
                    send_sem=send_sem.at[0, side], recv_sem=recv_sem.at[0, 1 - side],
                    device_id=(target,), device_id_type=MESH,
                ))
                copies[-1].start()
        tables(pack, step, 0)
        packet.wait_recv()
        receive(step)
        tables(near, step, 1)
        spread_all(dst)
        if step == 0:
            loads[1].wait()
            loads[2].wait()
        for c in copies:
            c.wait_recv()
            c.wait_send()
        advance(0, src, dst, outer(step, 0), inner(src, 1))
        advance(3, src, dst, inner(src, 2), outer(step, 1))
        if step + 1 < STEPS:
            copies = []
            for side, plane, target in ((0, 0, left), (1, 3, right)):
                copies.append(pltpu.make_async_remote_copy(
                    src_ref=low.at[plane], dst_ref=halo.at[step + 1, 1 - side],
                    send_sem=send_sem.at[step + 1, side], recv_sem=recv_sem.at[step + 1, 1 - side],
                    device_id=(target,), device_id_type=MESH,
                ))
        advance(1, src, dst, inner(src, 0), inner(src, 2))
        if step + 1 < STEPS:
            for c in copies:
                c.start()
        advance(2, src, dst, inner(src, 1), inner(src, 3))
        if step + 1 == STEPS:
            stores = [pltpu.make_async_copy(state.at[dst, p], vout.at[:, p], out_sem.at[p]) for p in range(CZ)]
            for c in stores:
                c.start()

        def near_sample(z, acc):
            return acc + sample(z, other)

        ret[step, 0:3, :] = lax.fori_loop(0, CZ - 1, near_sample, jnp.zeros((3, M), F32))
        acc = sample(0, own)
        answer = pltpu.make_async_remote_copy(
            src_ref=ret.at[step], dst_ref=back.at[step],
            send_sem=rsend.at[step], recv_sem=rrecv.at[step],
            device_id=(left,), device_id_type=MESH,
        )
        answer.start()
        acc = lax.fori_loop(1, CZ, lambda z, a: a + sample(z, own), acc)
        answer.wait_recv()
        offs[...] = offs[...] + DT * (living * (acc + back[step, 0:3, :]))
        waits += [packet, answer]
    oout[...] = offs[...]
    for c in waits:
        c.wait_send()
    for c in stores:
        c.wait()


def local(velocity, offsets, bases, targets, stiffness, active_block_count):
    vmem = pl.BlockSpec(memory_space=pltpu.VMEM)
    hbm = pl.BlockSpec(memory_space=pl.ANY)
    return pl.pallas_call(
        kernel,
        out_shape=(
            jax.ShapeDtypeStruct(velocity.shape, F32),
            jax.ShapeDtypeStruct(offsets.shape, F32),
        ),
        in_specs=[hbm, vmem, vmem, vmem, vmem, vmem],
        out_specs=(hbm, vmem),
        scratch_shapes=[
            pltpu.VMEM((2, CZ, 3, NY, NX), F32),
            pltpu.VMEM((CZ, 3, NY, NX), BF),
            pltpu.VMEM((2, 3, NY, NX), BF),
            pltpu.VMEM((STEPS, 2, 3, NY, NX), BF),
            pltpu.VMEM((NX, 2 * M), BF),
            pltpu.VMEM((NY, 2 * M), F32),
            pltpu.VMEM((3 * NY, 2 * M), BF),
            pltpu.VMEM((CZ, 8, 2 * M), F32),
            pltpu.VMEM((CZ, 8, 2 * M), F32),
            pltpu.VMEM((STEPS, 16, M), F32),
            pltpu.VMEM((STEPS, 16, M), F32),
            pltpu.VMEM((STEPS, 8, M), F32),
            pltpu.VMEM((STEPS, 8, M), F32),
            pltpu.VMEM((3, M), F32),
            pltpu.SemaphoreType.DMA((CZ,)),
            pltpu.SemaphoreType.DMA((CZ,)),
            pltpu.SemaphoreType.DMA((STEPS, 2)),
            pltpu.SemaphoreType.DMA((STEPS, 2)),
            pltpu.SemaphoreType.DMA((STEPS,)),
            pltpu.SemaphoreType.DMA((STEPS,)),
            pltpu.SemaphoreType.DMA((STEPS,)),
            pltpu.SemaphoreType.DMA((STEPS,)),
        ],
        compiler_params=pltpu.CompilerParams(
            collective_id=0, has_side_effects=True, vmem_limit_bytes=60 * 1024 * 1024
        ),
    )(
        velocity,
        offsets,
        bases,
        targets,
        stiffness.reshape(1, -1),
        active_block_count.reshape(1, 1),
    )


def solution(mesh):
    return jax.shard_map(
        local,
        mesh=mesh,
        in_specs=(
            P(None, AXIS, None, None),
            P(None, AXIS),
            P(None, AXIS),
            P(None, AXIS),
            P(AXIS),
            P(AXIS),
        ),
        out_specs=(P(None, AXIS, None, None), P(None, AXIS)),
        check_vma=False,
    )
```

```python
import functools
import math

import jax
import jax.numpy as jnp
from jax import lax
from jax.experimental import pallas as pl
from jax.experimental.pallas import tpu as pltpu
from jax.sharding import PartitionSpec as P

AXIS = "gz"
BLK = 256
STEPS = 2
DT = 0.2
NU = 0.3
CZ = 4
NY = 256
NX = 512
M = 512
MESH = pl.DeviceIdType.MESH
BF = jnp.bfloat16
F32 = jnp.float32


def weights(offsets):
    angle = offsets * (0.5 * math.pi)
    c = 0.25 * jnp.cos(angle)
    s = 0.25 * jnp.sin(angle)
    return (0.25 + c, 0.25 + s, 0.25 - c, 0.25 - s)


def pick(delta, taps):
    out = jnp.where(delta == 3, taps[3], 0.0)
    for j in (2, 1, 0):
        out = jnp.where(delta == j, taps[j], out)
    return out


def kernel(
    vel, off_in, bases_in, targ_in, stiff_in, act_in,
    vout, oout,
    spare, low, edge, halo, xtab, ytab, lhs, gains, zrows, pack, near, ret, back, offs, off_ref, bases_ref, targ_ref, stiff_ref, act_ref,
    in_sem, small_sem, send_sem, recv_sem, psend, precv, rsend, rrecv,
):
    state = (vout, spare)
    me = lax.axis_index(AXIS)
    count = lax.axis_size(AXIS)
    right = lax.rem(me + 1, count)
    left = lax.rem(me + count - 1, count)

    smalls = [
        pltpu.make_async_copy(a, b, small_sem.at[i])
        for i, (a, b) in enumerate((
            (off_in, off_ref), (bases_in, bases_ref), (targ_in, targ_ref),
            (stiff_in, stiff_ref), (act_in, act_ref),
        ))
    ]
    for copy in smalls:
        copy.start()
    loads = {}
    for p in (0, 3, 1, 2):
        loads[p] = pltpu.make_async_copy(vel.at[:, p], vout.at[:, p], in_sem.at[p])
        loads[p].start()

    barrier = pltpu.get_barrier_semaphore()
    for neighbour in (left, right):
        pl.semaphore_signal(barrier, inc=1, device_id=(neighbour,), device_id_type=MESH)

    for copy in smalls:
        copy.wait()
    lane = lax.broadcasted_iota(jnp.int32, (1, M), 1)
    living = jnp.where(lane < act_ref[...] * BLK, 1.0, 0.0)
    strength = living * stiff_ref[...]
    level = bases_ref[2:3, :] - me * CZ
    offs[...] = off_ref[...]

    def prepare(slot):
        o = offs[...]
        w = weights(o)
        force = strength * (targ_ref[...] - o)
        for j in range(4):
            pack[slot, 6 + j : 7 + j, :] = w[j][0:1]
            pack[slot, 10 + j : 11 + j, :] = w[j][1:2]
        pack[slot, 0:3, :] = force
        pack[slot, 14:16, :] = bases_ref[0:2, :].astype(F32)
        for z in range(7):
            row = pick(z - level, [w[j][2:3] for j in range(4)])
            if z < CZ:
                zrows[z, 0:1, 0:M] = row
                gains[z, 0:3, 0:M] = force * row
            else:
                pack[slot, 3 + z - CZ : 4 + z - CZ, :] = row

    def receive(slot):
        zrows[CZ - 1, 0:1, M:] = jnp.zeros((1, M), F32)
        gains[CZ - 1, 0:3, M:] = jnp.zeros((3, M), F32)
        for z in range(3):
            row = near[slot, 3 + z : 4 + z, :]
            zrows[z, 0:1, M:] = row
            gains[z, 0:3, M:] = near[slot, 0:3, :] * row

    def tables(source, slot, side):
        lanes = pl.ds(side * M, M)

        def xrow(i, _):
            r = pl.multiple_of(i * 16, 16)
            where = lax.broadcasted_iota(jnp.int32, (16, M), 0) + r
            delta = (where - source[slot, 14:15, :].astype(jnp.int32)) & (NX - 1)
            taps = [source[slot, 6 + j : 7 + j, :] for j in range(4)]
            xtab[pl.ds(r, 16), lanes] = pick(delta, taps).astype(BF)
            return 0

        lax.fori_loop(0, NX // 16, xrow, 0)

        def yrow(i, _):
            r = pl.multiple_of(i * 16, 16)
            where = lax.broadcasted_iota(jnp.int32, (16, M), 0) + r
            delta = (where - source[slot, 15:16, :].astype(jnp.int32)) & (NY - 1)
            taps = [source[slot, 10 + j : 11 + j, :] for j in range(4)]
            ytab[pl.ds(r, 16), lanes] = pick(delta, taps)
            return 0

        lax.fori_loop(0, NY // 16, yrow, 0)

    core = lax.rem(me, 2)
    partner = (me + 1 - 2 * core, lax.rem(me + count - 1 + 2 * core, count))
    plane = (3 - 3 * core, 3 * core)
    inside = (2 - core, 1 + core)
    side = 1.0 - 2.0 * core.astype(F32)
    sides = (side, -side)

    def stencil(p, src, dst, near_planes, sign=None):
        def rows(i, _):
            r = pl.multiple_of(i * 16, 16)
            rp = pl.multiple_of(lax.rem(r + NY - 8, NY), 8)
            rn = pl.multiple_of(lax.rem(r + 16, NY), 8)
            adjacent = [near_planes(c, pl.ds(r, 16)) for c in range(3)]
            tiles = [
                [src[c, p, pl.ds(rp, 8), :], src[c, p, pl.ds(r, 8), :],
                 src[c, p, pl.ds(r + 8, 8), :], src[c, p, pl.ds(rn, 8), :]]
                for c in range(3)
            ]
            for h in (0, 1):
                upper, lower = [], []
                for d in (2, 1, 0):
                    scaled = (0.5 * DT) * tiles[d][1 + h]
                    if d == 2 and sign is not None:
                        scaled = sign * scaled
                    upper.append(DT * NU - scaled)
                    lower.append(DT * NU + scaled)
                for c in range(3):
                    prev, v, nxt = tiles[c][h], tiles[c][h + 1], tiles[c][h + 2]
                    above, below = (x[8 * h : 8 * h + 8] for x in adjacent[c])
                    yup = pltpu.roll(jnp.concatenate([v, nxt], axis=0), 15, 0)[0:8]
                    ydown = pltpu.roll(jnp.concatenate([prev, v], axis=0), 1, 0)[8:16]
                    total = (1.0 - 6.0 * DT * NU) * v
                    total = total + upper[0] * above + lower[0] * below
                    total = total + upper[1] * yup + lower[1] * ydown
                    total = total + upper[2] * pltpu.roll(v, NX - 1, 1) + lower[2] * pltpu.roll(v, 1, 1)
                    dst[c, p, pl.ds(r + 8 * h, 8), :] = total
            return 0

        lax.fori_loop(0, NY // 16, rows, 0)

    def interior(src, dst):
        for p in (1, 2):
            stencil(p, src, dst, lambda c, rows: (src[c, p + 1, rows, :], src[c, p - 1, rows, :]))

    def border(k, step, src, dst):
        stencil(
            plane[k], src, dst,
            lambda c, rows: (halo[step, k, c, rows, :].astype(F32), src[c, inside[k], rows, :]),
            sides[k],
        )

    def spread(z, dst):
        for c in range(3):
            lhs[c * NY : (c + 1) * NY, :] = (gains[z, c : c + 1, :] * ytab[...]).astype(BF)
        out = lax.dot_general(
            lhs[...], xtab[...], (((1,), (1,)), ((), ())), preferred_element_type=F32
        )
        total = dst[:, z] + DT * out.reshape(3, NY, NX)
        dst[:, z] = total
        low[z] = total.astype(BF)

    def sample(z, lanes):
        out = jnp.dot(low[z].reshape(3 * NY, NX), xtab[:, lanes], preferred_element_type=F32)
        y = ytab[:, lanes]
        parts = [jnp.sum(out[c * NY : (c + 1) * NY] * y, axis=0, keepdims=True) for c in range(3)]
        return jnp.concatenate(parts, axis=0) * zrows[z, 0:1, lanes]

    own = slice(0, M)
    other = slice(M, 2 * M)

    def sending(step, k, ref):
        return pltpu.make_async_remote_copy(
            src_ref=ref, dst_ref=halo.at[step, k],
            send_sem=send_sem.at[step, k], recv_sem=recv_sem.at[step, k],
            device_id=(partner[k],), device_id_type=MESH,
        )

    waits = []
    for step in range(STEPS):
        src, dst = state[step % 2], state[(step + 1) % 2]
        prepare(step)
        if step == 0:
            loads[0].wait()
            loads[3].wait()
            for k in (1, 0):

                def lower_rows(i, _, k=k):
                    r = pl.multiple_of(i * 16, 16)
                    for c in range(3):
                        edge[k, c, pl.ds(r, 16), :] = vout[c, plane[k], pl.ds(r, 16), :].astype(BF)
                    return 0

                lax.fori_loop(0, NY // 16, lower_rows, 0)
            pl.semaphore_wait(barrier, 2)
        packet = pltpu.make_async_remote_copy(
            src_ref=pack.at[step], dst_ref=near.at[step],
            send_sem=psend.at[step], recv_sem=precv.at[step],
            device_id=(right,), device_id_type=MESH,
        )
        packet.start()
        if step == 0:
            copies = [sending(0, k, edge.at[k]) for k in range(2)]
            copies[1].start()
            copies[0].start()
        tables(pack, step, 0)
        if step == 0:
            loads[1].wait()
            loads[2].wait()
            interior(src, dst)
        copies[0].wait()
        border(0, step, src, dst)
        packet.wait_recv()
        receive(step)
        tables(near, step, 1)

        def two(z, _):
            spread(z, dst)
            return 0

        lax.fori_loop(1, 3, two, 0)
        spread(plane[0], dst)
        if step + 1 < STEPS:
            after = [sending(step + 1, k, low.at[plane[k]]) for k in range(2)]
        copies[1].wait()
        border(1, step, src, dst)
        spread(plane[1], dst)
        if step + 1 < STEPS:
            after[1].start()
            after[0].start()
            copies = after

        def near_sample(z, acc):
            return acc + sample(z, other)

        ret[step, 0:3, :] = lax.fori_loop(0, CZ - 1, near_sample, jnp.zeros((3, M), F32))
        acc = sample(0, own)
        answer = pltpu.make_async_remote_copy(
            src_ref=ret.at[step], dst_ref=back.at[step],
            send_sem=rsend.at[step], recv_sem=rrecv.at[step],
            device_id=(left,), device_id_type=MESH,
        )
        answer.start()
        acc = lax.fori_loop(1, CZ, lambda z, a: a + sample(z, own), acc)
        if step + 1 < STEPS:
            interior(dst, src)
        answer.wait_recv()
        offs[...] = offs[...] + DT * (living * (acc + back[step, 0:3, :]))
        waits += [packet, answer]
    oout[...] = offs[...]
    for c in waits:
        c.wait_send()


def local(velocity, offsets, bases, targets, stiffness, active_block_count):
    vmem = pl.BlockSpec(memory_space=pltpu.VMEM)
    hbm = pl.BlockSpec(memory_space=pltpu.HBM)
    return pl.pallas_call(
        kernel,
        out_shape=(
            jax.ShapeDtypeStruct(velocity.shape, F32),
            jax.ShapeDtypeStruct(offsets.shape, F32),
        ),
        in_specs=[hbm] * 6,
        out_specs=(vmem, vmem),
        scratch_shapes=[
            pltpu.VMEM((3, CZ, NY, NX), F32),
            pltpu.VMEM((CZ, 3, NY, NX), BF),
            pltpu.VMEM((2, 3, NY, NX), BF),
            pltpu.VMEM((STEPS, 2, 3, NY, NX), BF),
            pltpu.VMEM((NX, 2 * M), BF),
            pltpu.VMEM((NY, 2 * M), F32),
            pltpu.VMEM((3 * NY, 2 * M), BF),
            pltpu.VMEM((CZ, 8, 2 * M), F32),
            pltpu.VMEM((CZ, 8, 2 * M), F32),
            pltpu.VMEM((STEPS, 16, M), F32),
            pltpu.VMEM((STEPS, 16, M), F32),
            pltpu.VMEM((STEPS, 8, M), F32),
            pltpu.VMEM((STEPS, 8, M), F32),
            pltpu.VMEM((3, M), F32),
            pltpu.VMEM((3, M), F32),
            pltpu.VMEM((3, M), jnp.int32),
            pltpu.VMEM((3, M), F32),
            pltpu.VMEM((1, M), F32),
            pltpu.VMEM((1, 1), jnp.int32),
            pltpu.SemaphoreType.DMA((CZ,)),
            pltpu.SemaphoreType.DMA((5,)),
            pltpu.SemaphoreType.DMA((STEPS, 2)),
            pltpu.SemaphoreType.DMA((STEPS, 2)),
            pltpu.SemaphoreType.DMA((STEPS,)),
            pltpu.SemaphoreType.DMA((STEPS,)),
            pltpu.SemaphoreType.DMA((STEPS,)),
            pltpu.SemaphoreType.DMA((STEPS,)),
        ],
        compiler_params=pltpu.CompilerParams(
            collective_id=0, has_side_effects=True, vmem_limit_bytes=40 * 1024 * 1024
        ),
    )(*(
        pltpu.with_memory_space_constraint(a, pltpu.HBM)
        for a in (
            velocity,
            offsets,
            bases,
            targets,
            stiffness.reshape(1, -1),
        )
    ), active_block_count.reshape(1, 1))


def solution(mesh):
    return jax.shard_map(
        local,
        mesh=mesh,
        in_specs=(
            P(None, AXIS, None, None),
            P(None, AXIS),
            P(None, AXIS),
            P(None, AXIS),
            P(AXIS),
            P(AXIS),
        ),
        out_specs=(P(None, AXIS, None, None), P(None, AXIS)),
        check_vma=False,
    )
```

```python
import math

import jax
import jax.numpy as jnp
from jax import lax
from jax.experimental import pallas as pl
from jax.experimental.pallas import tpu as pltpu
from jax.sharding import PartitionSpec as P

AXIS = "gz"
BLK = 256
STEPS = 2
DT = 0.2
NU = 0.3
CZ = 4
NY = 256
NX = 512
M = 512
LB = NX // 128
MESH = pl.DeviceIdType.MESH
BF = jnp.bfloat16
F32 = jnp.float32


def weights(offsets):
    angle = offsets * (0.5 * math.pi)
    c = 0.25 * jnp.cos(angle)
    s = 0.25 * jnp.sin(angle)
    return (0.25 + c, 0.25 + s, 0.25 - c, 0.25 - s)


def pick(delta, taps):
    out = jnp.where(delta == 3, taps[3], 0.0)
    for j in (2, 1, 0):
        out = jnp.where(delta == j, taps[j], out)
    return out


def kernel(
    vel, off_in, bases_in, targ_in, stiff_in, act_in,
    vout, oout,
    first, second, low, edge, halo, xtab, ytab, lhs, gains, zrows, taps, cells, marks, pack, near,
    part, got, offs, bases_ref, targ_ref, stiff_ref, act_ref,
    in_sem, small_sem, send_sem, recv_sem, psend, precv, rsend, rrecv,
):
    me = lax.axis_index(AXIS)
    count = lax.axis_size(AXIS)
    right = lax.rem(me + 1, count)
    left = lax.rem(me + count - 1, count)

    smalls = [
        pltpu.make_async_copy(a, b, small_sem.at[i])
        for i, (a, b) in enumerate((
            (off_in, offs), (bases_in, bases_ref), (targ_in, targ_ref),
            (stiff_in, stiff_ref), (act_in, act_ref),
        ))
    ]
    for copy in smalls:
        copy.start()
    loads = {}
    for p in (0, 3, 1, 2):
        loads[p] = []
        for b in range(LB):
            lanes = pl.ds(b * 128, 128)
            for j, (rows, to) in enumerate((
                (pl.ds(0, NY), pl.ds(8, NY)),
                (pl.ds(NY - 8, 8), pl.ds(0, 8)),
                (pl.ds(0, 8), pl.ds(NY + 8, 8)),
            )):
                loads[p].append(pltpu.make_async_copy(
                    vel.at[:, p, rows, lanes], first.at[:, p, b, to, :], in_sem.at[p, b, j]
                ))
                loads[p][-1].start()

    barrier = pltpu.get_barrier_semaphore()
    for neighbour in (left, right):
        pl.semaphore_signal(barrier, inc=1, device_id=(neighbour,), device_id_type=MESH)

    for copy in smalls:
        copy.wait()
    lane = lax.broadcasted_iota(jnp.int32, (1, M), 1)
    living = jnp.where(lane < act_ref[...] * BLK, 1.0, 0.0)
    pack[0:3, :] = offs[...]
    pack[3:6, :] = targ_ref[...]
    pack[6:7, :] = living * stiff_ref[...]
    pack[7:8, :] = living
    pack[8:10, :] = bases_ref[0:2, :].astype(F32)
    pack[10:11, :] = (bases_ref[2:3, :] - me * CZ).astype(F32)
    pack[11:16, :] = jnp.zeros((5, M), F32)

    def prepare():
        o = marks[0:3, :]
        w = weights(o)
        force = marks[6:7, :] * (marks[3:6, :] - o)
        for j in range(4):
            taps[j : j + 1, :] = w[j][0:1]
            taps[4 + j : 5 + j, :] = w[j][1:2]
        for z in range(CZ):
            row = pick(z - cells[2:3, :], [w[j][2:3] for j in range(4)])
            zrows[z, 0:1, :] = row
            gains[z, 0:3, :] = force * row

    def tables():
        def xrow(i, _):
            r = pl.multiple_of(i * 16, 16)
            for half in (slice(0, M), slice(M, 2 * M)):
                where = lax.broadcasted_iota(jnp.int32, (16, M), 0) + r
                delta = (where - cells[0:1, half]) & (NX - 1)
                xtab[pl.ds(r, 16), half] = pick(delta, [taps[j : j + 1, half] for j in range(4)]).astype(BF)
            return 0

        lax.fori_loop(0, NX // 16, xrow, 0)

        def yrow(i, _):
            r = pl.multiple_of(i * 16, 16)
            for half in (slice(0, M), slice(M, 2 * M)):
                where = lax.broadcasted_iota(jnp.int32, (16, M), 0) + r
                delta = (where - cells[1:2, half]) & (NY - 1)
                ytab[pl.ds(r, 16), half] = pick(delta, [taps[4 + j : 5 + j, half] for j in range(4)])
            return 0

        lax.fori_loop(0, NY // 16, yrow, 0)

    core = lax.rem(me, 2)
    partner = (me + 1 - 2 * core, lax.rem(me + count - 1 + 2 * core, count))
    plane = (3 - 3 * core, 3 * core)
    inside = (2 - core, 1 + core)
    side = 1.0 - 2.0 * core.astype(F32)
    sides = (side, -side)

    lane128 = lax.broadcasted_iota(jnp.int32, (16, 128), 1)


    def stencil(p0, planes, src, put, near_planes, sign=None):
        per = NY // 64

        def rows(i, _):
            p = p0 + i // per
            base = pl.multiple_of((i % per) * 64, 64)
            for h in range(64 // 16):
                r = base + 16 * h
                turned = []
                for c in range(3):
                    v = [src[c, p, b, pl.ds(r + 8, 16), :] for b in range(LB)]
                    up = [pltpu.roll(x, 127, 1) for x in v]
                    down = [pltpu.roll(x, 1, 1) for x in v]
                    turned.append((
                        [jnp.where(lane128 == 127, up[(b + 1) % LB], up[b]) for b in range(LB)],
                        [jnp.where(lane128 == 0, down[(b - 1) % LB], down[b]) for b in range(LB)],
                    ))
                for b in range(LB):
                    v = [src[c, p, b, pl.ds(r + 8, 16), :] for c in range(3)]
                    upper, lower = [], []
                    for d in (2, 1, 0):
                        scaled = (0.5 * DT) * v[d]
                        if d == 2 and sign is not None:
                            scaled = sign * scaled
                        upper.append(DT * NU - scaled)
                        lower.append(DT * NU + scaled)
                    for c in range(3):
                        above, below = near_planes(c, p, b, r)
                        total = (1.0 - 6.0 * DT * NU) * v[c]
                        total = total + (upper[0] * above + lower[0] * below)
                        total = total + (
                            upper[1] * src[c, p, b, pl.ds(r + 9, 16), :]
                            + lower[1] * src[c, p, b, pl.ds(r + 7, 16), :]
                        )
                        total = total + (upper[2] * turned[c][0][b] + lower[2] * turned[c][1][b])
                        put(c, p, b, r, total)
            return 0

        lax.fori_loop(0, per * planes, rows, 0)

    def putter(step):
        def to_second(c, p, b, r, total):
            second[c, p, b, pl.ds(r + 8, 16), :] = total

        def to_output(c, p, b, r, total):
            vout[c, p, pl.ds(r, 16), b * 128 : b * 128 + 128] = total

        return to_second if step == 0 else to_output

    source = (first, second)

    def interior(step):
        src = source[step]
        stencil(
            1, 2, src, putter(step),
            lambda c, p, b, r: (
                src[c, p + 1, b, pl.ds(r + 8, 16), :], src[c, p - 1, b, pl.ds(r + 8, 16), :]
            ),
        )

    def border(k, step):
        src = source[step]
        stencil(
            plane[k], 1, src, putter(step),
            lambda c, p, b, r: (
                halo[step, k, c, pl.ds(r, 16), b * 128 : b * 128 + 128].astype(F32),
                src[c, inside[k], b, pl.ds(r + 8, 16), :],
            ),
            sides[k],
        )

    def spread(z, step):
        for c in range(3):
            lhs[c * NY : (c + 1) * NY, :] = (gains[z, c : c + 1, :] * ytab[...]).astype(BF)
        out = lax.dot_general(
            lhs[...], xtab[...], (((1,), (1,)), ((), ())), preferred_element_type=F32
        ).reshape(3, NY, NX)
        for b in range(LB):
            lanes = slice(b * 128, b * 128 + 128)
            if step == 0:
                total = second[:, z, b, 8 : NY + 8, :] + DT * out[:, :, lanes]
                second[:, z, b, 8 : NY + 8, :] = total
                second[:, z, b, 0:8, :] = total[:, NY - 8 :]
                second[:, z, b, NY + 8 :, :] = total[:, :8]
            else:
                total = vout[:, z, :, lanes] + DT * out[:, :, lanes]
                vout[:, z, :, lanes] = total
            low[z, :, :, lanes] = total.astype(BF)

    def sample(z):
        out = jnp.dot(low[z].reshape(3 * NY, NX), xtab[...], preferred_element_type=F32)
        y = ytab[...]
        parts = [jnp.sum(out[c * NY : (c + 1) * NY] * y, axis=0, keepdims=True) for c in range(3)]
        return jnp.concatenate(parts, axis=0) * zrows[z, 0:1, :]

    def sending(step, k, ref):
        return pltpu.make_async_remote_copy(
            src_ref=ref, dst_ref=halo.at[step, k],
            send_sem=send_sem.at[step, k], recv_sem=recv_sem.at[step, k],
            device_id=(partner[k],), device_id_type=MESH,
        )

    packet = pltpu.make_async_remote_copy(
        src_ref=pack, dst_ref=near, send_sem=psend, recv_sem=precv,
        device_id=(right,), device_id_type=MESH,
    )
    for c in loads[0] + loads[3]:
        c.wait()
    copies = [sending(0, k, edge.at[k]) for k in range(2)]
    for k in (1, 0):

        def lower_rows(i, _, k=k):
            r = pl.multiple_of(i * 16, 16)
            for c in range(3):
                for b in range(LB):
                    edge[k, c, pl.ds(r, 16), b * 128 : b * 128 + 128] = (
                        first[c, plane[k], b, pl.ds(r + 8, 16), :].astype(BF)
                    )
            return 0

        lax.fori_loop(0, NY // 16, lower_rows, 0)
        if k == 1:
            pl.semaphore_wait(barrier, 2)
            packet.start()
    copies[1].start()
    copies[0].start()
    for c in loads[1] + loads[2]:
        c.wait()
    interior(0)
    packet.wait_recv()
    marks[:, 0:M] = pack[...]
    marks[:, M:] = near[...]
    cells[0:2, :] = marks[8:10, :].astype(jnp.int32)
    cells[2:3, 0:M] = pack[10:11, :].astype(jnp.int32)
    cells[2:3, M:] = near[10:11, :].astype(jnp.int32) - CZ

    waits = [packet]
    for step in range(STEPS):
        last = step + 1 == STEPS
        prepare()
        tables()
        copies[0].wait()
        border(0, step)
        after = [] if last else [sending(step + 1, k, low.at[plane[k]]) for k in range(2)]

        def spread_one(i, _):
            spread(jnp.where(i == 2, plane[0], i + 1), step)
            return 0

        def sample_one(i, acc):
            return acc + sample(jnp.where(i == 2, plane[0], i + 1))

        lax.fori_loop(0, 3, spread_one, 0)
        if not last:
            after[0].start()
        acc = lax.fori_loop(0, 3, sample_one, jnp.zeros((3, 2 * M), F32))
        copies[1].wait()
        border(1, step)
        spread(plane[1], step)
        acc = acc + sample(plane[1])
        part[step, 0, 0:3, :] = acc[:, :M]
        part[step, 1, 0:3, :] = acc[:, M:]
        answers = [
            pltpu.make_async_remote_copy(
                src_ref=part.at[step, k], dst_ref=got.at[step, k],
                send_sem=rsend.at[step, k], recv_sem=rrecv.at[step, k],
                device_id=(target,), device_id_type=MESH,
            )
            for k, target in ((1, left), (0, right))[: 1 if last else 2]
        ]
        for c in answers:
            c.start()
        if not last:
            after[1].start()
            copies = after
            interior(step + 1)
        for c in answers:
            c.wait_recv()
        if last:
            oout[...] = marks[0:3, 0:M] + DT * (marks[7:8, 0:M] * (acc[:, :M] + got[step, 1, 0:3, :]))
        else:
            marks[0:3, 0:M] = marks[0:3, 0:M] + DT * (
                marks[7:8, 0:M] * (part[step, 0, 0:3, :] + got[step, 1, 0:3, :])
            )
            marks[0:3, M:] = marks[0:3, M:] + DT * (
                marks[7:8, M:] * (got[step, 0, 0:3, :] + part[step, 1, 0:3, :])
            )
        waits += answers
    for c in waits:
        c.wait_send()


def local(velocity, offsets, bases, targets, stiffness, active_block_count):
    vmem = pl.BlockSpec(memory_space=pltpu.VMEM)
    hbm = pl.BlockSpec(memory_space=pltpu.HBM)
    return pl.pallas_call(
        kernel,
        out_shape=(
            jax.ShapeDtypeStruct(velocity.shape, F32),
            jax.ShapeDtypeStruct(offsets.shape, F32),
        ),
        in_specs=[hbm] * 6,
        out_specs=(vmem, vmem),
        scratch_shapes=[
            pltpu.VMEM((3, CZ, LB, NY + 16, 128), F32),
            pltpu.VMEM((3, CZ, LB, NY + 16, 128), F32),
            pltpu.VMEM((CZ, 3, NY, NX), BF),
            pltpu.VMEM((2, 3, NY, NX), BF),
            pltpu.VMEM((STEPS, 2, 3, NY, NX), BF),
            pltpu.VMEM((NX, 2 * M), BF),
            pltpu.VMEM((NY, 2 * M), F32),
            pltpu.VMEM((3 * NY, 2 * M), BF),
            pltpu.VMEM((CZ, 8, 2 * M), F32),
            pltpu.VMEM((CZ, 8, 2 * M), F32),
            pltpu.VMEM((8, 2 * M), F32),
            pltpu.VMEM((8, 2 * M), jnp.int32),
            pltpu.VMEM((16, 2 * M), F32),
            pltpu.VMEM((16, M), F32),
            pltpu.VMEM((16, M), F32),
            pltpu.VMEM((STEPS, 2, 8, M), F32),
            pltpu.VMEM((STEPS, 2, 8, M), F32),
            pltpu.VMEM((3, M), F32),
            pltpu.VMEM((3, M), jnp.int32),
            pltpu.VMEM((3, M), F32),
            pltpu.VMEM((1, M), F32),
            pltpu.VMEM((1, 1), jnp.int32),
            pltpu.SemaphoreType.DMA((CZ, LB, 3)),
            pltpu.SemaphoreType.DMA((5,)),
            pltpu.SemaphoreType.DMA((STEPS, 2)),
            pltpu.SemaphoreType.DMA((STEPS, 2)),
            pltpu.SemaphoreType.DMA,
            pltpu.SemaphoreType.DMA,
            pltpu.SemaphoreType.DMA((STEPS, 2)),
            pltpu.SemaphoreType.DMA((STEPS, 2)),
        ],
        compiler_params=pltpu.CompilerParams(
            collective_id=0, has_side_effects=True, vmem_limit_bytes=40 * 1024 * 1024
        ),
    )(*(
        pltpu.with_memory_space_constraint(a, pltpu.HBM)
        for a in (
            velocity,
            offsets,
            bases,
            targets,
            stiffness.reshape(1, -1),
        )
    ), active_block_count.reshape(1, 1))


def solution(mesh):
    return jax.shard_map(
        local,
        mesh=mesh,
        in_specs=(
            P(None, AXIS, None, None),
            P(None, AXIS),
            P(None, AXIS),
            P(None, AXIS),
            P(AXIS),
            P(AXIS),
        ),
        out_specs=(P(None, AXIS, None, None), P(None, AXIS)),
        check_vma=False,
    )
```

```python
import math

import jax
import jax.numpy as jnp
from jax import lax
from jax.experimental import pallas as pl
from jax.experimental.pallas import tpu as pltpu
from jax.sharding import PartitionSpec as P

AXIS = "gz"
BLK = 256
STEPS = 2
DT = 0.2
NU = 0.3
CZ = 4
NY = 256
NX = 512
M = 512
LB = NX // 128
MESH = pl.DeviceIdType.MESH
BF = jnp.bfloat16
F32 = jnp.float32


def weights(offsets):
    angle = offsets * (0.5 * math.pi)
    c = 0.25 * jnp.cos(angle)
    s = 0.25 * jnp.sin(angle)
    return (0.25 + c, 0.25 + s, 0.25 - c, 0.25 - s)


def pick(delta, taps):
    out = jnp.where(delta == 3, taps[3], 0.0)
    for j in (2, 1, 0):
        out = jnp.where(delta == j, taps[j], out)
    return out


def kernel(
    vel, off_in, bases_in, targ_in, stiff_in, act_in,
    vout, oout,
    inner_a, outer_a, inner_b, outer_b, low, edge, halo, xtab, ytab, lhs, gains, zrows, taps, cells, marks, pack, near,
    sums, part, got, offs, bases_ref, targ_ref, stiff_ref, act_ref,
    in_sem, small_sem, send_sem, recv_sem, psend, precv, rsend, rrecv,
):
    me = lax.axis_index(AXIS)
    count = lax.axis_size(AXIS)
    right = lax.rem(me + 1, count)
    left = lax.rem(me + count - 1, count)

    smalls = [
        pltpu.make_async_copy(a, b, small_sem.at[i])
        for i, (a, b) in enumerate((
            (off_in, offs), (bases_in, bases_ref), (targ_in, targ_ref),
            (stiff_in, stiff_ref), (act_in, act_ref),
        ))
    ]
    for copy in smalls:
        copy.start()
    sets = ((inner_a, outer_a), (inner_b, outer_b))
    loads = {}
    for p in (0, 3, 1, 2):
        home, at = (outer_a, p // 3) if p in (0, 3) else (inner_a, p - 1)
        loads[p] = []
        for b in range(LB):
            lanes = pl.ds(b * 128, 128)
            for j, (rows, to) in enumerate((
                (pl.ds(0, NY), pl.ds(8, NY)),
                (pl.ds(NY - 8, 8), pl.ds(0, 8)),
                (pl.ds(0, 8), pl.ds(NY + 8, 8)),
            )):
                loads[p].append(pltpu.make_async_copy(
                    vel.at[:, p, rows, lanes], home.at[:, at, b, to, :], in_sem.at[p, b, j]
                ))
                loads[p][-1].start()

    barrier = pltpu.get_barrier_semaphore()
    for neighbour in (left, right):
        pl.semaphore_signal(barrier, inc=1, device_id=(neighbour,), device_id_type=MESH)

    for copy in smalls:
        copy.wait()
    lane = lax.broadcasted_iota(jnp.int32, (1, M), 1)
    living = jnp.where(lane < act_ref[...] * BLK, 1.0, 0.0)
    pack[0:3, :] = offs[...]
    pack[3:6, :] = targ_ref[...]
    pack[6:7, :] = living * stiff_ref[...]
    pack[7:8, :] = living
    pack[8:10, :] = bases_ref[0:2, :].astype(F32)
    pack[10:11, :] = (bases_ref[2:3, :] - me * CZ).astype(F32)
    pack[11:16, :] = jnp.zeros((5, M), F32)

    def prepare(half):
        o = marks[0:3, half]
        w = weights(o)
        force = marks[6:7, half] * (marks[3:6, half] - o)
        for j in range(4):
            taps[j : j + 1, half] = w[j][0:1]
            taps[4 + j : 5 + j, half] = w[j][1:2]
        for z in range(CZ):
            row = pick(z - cells[8:9, half], [w[j][2:3] for j in range(4)])
            zrows[z, 0:1, half] = row
            gains[z, 0:3, half] = force * row

    def tables(halves):
        def fill(table, extent, first, kind):
            def rows(i, _):
                r = pl.multiple_of(i * 32, 32)
                for half in halves:
                    where = lax.broadcasted_iota(jnp.int32, (32, M), 0) + r
                    out = 0.0
                    for j in range(4):
                        out = jnp.where(
                            where == cells[first + j : first + j + 1, half],
                            taps[first + j : first + j + 1, half],
                            out,
                        )
                    table[pl.ds(r, 32), half] = out.astype(kind)
                return 0

            lax.fori_loop(0, extent // 32, rows, 0)

        fill(xtab, NX, 0, BF)
        fill(ytab, NY, 4, F32)

    core = lax.rem(me, 2)
    partner = (me + 1 - 2 * core, lax.rem(me + count - 1 + 2 * core, count))
    plane = (3 - 3 * core, 3 * core)
    at = (1 - core, core)
    side = 1.0 - 2.0 * core.astype(F32)
    sides = (side, -side)
    lane128 = lax.broadcasted_iota(jnp.int32, (16, 128), 1)

    def stencil(src, dst, p, base, height, near_planes, sign=None):
        for h in range(height // 16):
            r = base + 16 * h
            turned = []
            for c in range(3):
                v = [src[c, p, b, pl.ds(r + 8, 16), :] for b in range(LB)]
                up = [pltpu.roll(x, 127, 1) for x in v]
                down = [pltpu.roll(x, 1, 1) for x in v]
                turned.append((
                    [jnp.where(lane128 == 127, up[(b + 1) % LB], up[b]) for b in range(LB)],
                    [jnp.where(lane128 == 0, down[(b - 1) % LB], down[b]) for b in range(LB)],
                ))
            for b in range(LB):
                v = [src[c, p, b, pl.ds(r + 8, 16), :] for c in range(3)]
                upper, lower = [], []
                for d in (2, 1, 0):
                    scaled = (0.5 * DT) * v[d]
                    if d == 2 and sign is not None:
                        scaled = sign * scaled
                    upper.append(DT * NU - scaled)
                    lower.append(DT * NU + scaled)
                for c in range(3):
                    above, below = near_planes(c, b, r)
                    total = (1.0 - 6.0 * DT * NU) * v[c]
                    total = total + (upper[0] * above + lower[0] * below)
                    total = total + (
                        upper[1] * src[c, p, b, pl.ds(r + 9, 16), :]
                        + lower[1] * src[c, p, b, pl.ds(r + 7, 16), :]
                    )
                    total = total + (upper[2] * turned[c][0][b] + lower[2] * turned[c][1][b])
                    dst[c, p, b, pl.ds(r + 8, 16), :] = total

    def interior(step):
        (inn, out), (dst, _) = sets[step], sets[1 - step]
        for q in (0, 1):

            def near_planes(c, b, r, q=q):
                middle = inn[c, 1 - q, b, pl.ds(r + 8, 16), :]
                edge_plane = out[c, q, b, pl.ds(r + 8, 16), :]
                return (edge_plane, middle) if q else (middle, edge_plane)

            def rows(i, _, q=q, near_planes=near_planes):
                stencil(inn, dst, q, pl.multiple_of(i * 128, 128), 128, near_planes)
                return 0

            lax.fori_loop(0, NY // 128, rows, 0)

    def border(k, step, start, stop):
        (inn, out), (_, dst) = sets[step], sets[1 - step]

        def near_planes(c, b, r):
            return (
                halo[step, k, c, pl.ds(r, 16), b * 128 : b * 128 + 128].astype(F32),
                inn[c, at[k], b, pl.ds(r + 8, 16), :],
            )

        def rows(i, _):
            stencil(out, dst, at[k], pl.multiple_of(i * 128, 128), 128, near_planes, sides[k])
            return 0

        lax.fori_loop(start // 128, stop // 128, rows, 0)

    def spread(z, kind, q, step, start=0, stop=NY, width=2 * M):
        work = sets[1 - step][kind]
        height = stop - start
        for c in range(3):
            lhs[c * height : (c + 1) * height, 0:width] = (
                gains[z, c : c + 1, 0:width] * ytab[start:stop, 0:width]
            ).astype(BF)
        out = lax.dot_general(
            lhs[0 : 3 * height, 0:width],
            xtab[:, 0:width],
            (((1,), (1,)), ((), ())),
            preferred_element_type=F32,
        ).reshape(3, height, NX)
        for b in range(LB):
            lanes = slice(b * 128, b * 128 + 128)
            total = work[:, q, b, start + 8 : stop + 8, :] + DT * out[:, :, lanes]
            if step + 1 < STEPS:
                work[:, q, b, start + 8 : stop + 8, :] = total
                if stop == NY:
                    work[:, q, b, 0:8, :] = total[:, height - 8 :]
                if start == 0:
                    work[:, q, b, NY + 8 :, :] = total[:, :8]
            else:
                vout[:, z, start:stop, lanes] = total
            low[z, :, start:stop, lanes] = total.astype(BF)

    own, other = slice(0, M), slice(M, 2 * M)
    both = slice(0, 2 * M)

    def reduce_rows(out, z, half):
        y = ytab[:, half]
        parts = [jnp.sum(out[c * NY : (c + 1) * NY] * y, axis=0, keepdims=True) for c in range(3)]
        return jnp.concatenate(parts, axis=0) * zrows[z, 0:1, half]

    def sample(z, half=both):
        out = jnp.dot(low[z].reshape(3 * NY, NX), xtab[:, half], preferred_element_type=F32)
        return reduce_rows(out, z, half)

    def spread_outer(k, step, start, stop):
        @pl.when(core == k)
        def _():
            spread(CZ - 1, 1, 1, step, start, stop, M)

        @pl.when(core != k)
        def _():
            spread(0, 1, 0, step, start, stop)

    def sample_outer(k):
        @pl.when(core == k)
        def _():
            sums[0:3, own] = sums[0:3, own] + sample(CZ - 1, own)

        @pl.when(core != k)
        def _():
            sums[0:3, :] = sums[0:3, :] + sample(0)

    def sample_planes(planes, half):
        total = 0.0
        for z in range(planes):
            out = jnp.dot(low[z].reshape(3 * NY, NX), xtab[:, half], preferred_element_type=F32)
            total = total + reduce_rows(out, z, half)
        return total

    pieces = ((0, 0, NY), (1, 0, NY // 2), (1, NY // 2, NY))

    def sending(step, ref_of):
        out = []
        for i, (k, start, stop) in enumerate(pieces):
            rows = pl.ds(start, stop - start)
            out.append(pltpu.make_async_remote_copy(
                src_ref=ref_of(k).at[:, rows, :], dst_ref=halo.at[step, k, :, rows, :],
                send_sem=send_sem.at[step, i], recv_sem=recv_sem.at[step, i],
                device_id=(partner[k],), device_id_type=MESH,
            ))
        return out

    packet = pltpu.make_async_remote_copy(
        src_ref=pack, dst_ref=near, send_sem=psend, recv_sem=precv,
        device_id=(right,), device_id_type=MESH,
    )
    for c in loads[0] + loads[3]:
        c.wait()
    copies = sending(0, lambda k: edge.at[k])
    for k in (1, 0):

        def lower_rows(i, _, k=k):
            r = pl.multiple_of(i * 16, 16)
            for c in range(3):
                for b in range(LB):
                    edge[k, c, pl.ds(r, 16), b * 128 : b * 128 + 128] = (
                        outer_a[c, at[k], b, pl.ds(r + 8, 16), :].astype(BF)
                    )
            return 0

        lax.fori_loop(0, NY // 16, lower_rows, 0)
    pl.semaphore_wait(barrier, 2)
    packet.start()
    for i in (1, 0, 2):
        copies[i].start()
    for c in loads[1] + loads[2]:
        c.wait()
    interior(0)
    marks[:, own] = pack[...]

    def columns(half, shift):
        for j in range(4):
            cells[j : j + 1, half] = (marks[8:9, half].astype(jnp.int32) + j) & (NX - 1)
            cells[4 + j : 5 + j, half] = (marks[9:10, half].astype(jnp.int32) + j) & (NY - 1)
        cells[8:9, half] = marks[10:11, half].astype(jnp.int32) - shift

    waits = [packet]
    for step in range(STEPS):
        last = step + 1 == STEPS
        if step == 0:
            columns(own, 0)
            prepare(own)
            tables((own,))
            packet.wait_recv()
            marks[:, other] = near[...]
            columns(other, CZ)
            prepare(other)
            tables((other,))
        else:
            prepare(both)
            tables((own, other))
        copies[0].wait()
        border(0, step, 0, NY)
        after = [] if last else sending(step + 1, lambda k: low.at[plane[k]])

        def spread_one(i, _):
            spread(1 + i, 0, i, step)
            return 0

        def sample_one(i, acc):
            return acc + sample(1 + i)

        lax.fori_loop(0, 2, spread_one, 0)
        spread_outer(0, step, 0, NY)
        if not last:
            after[0].start()
        copies[1].wait()
        border(1, step, 0, NY // 2)
        spread_outer(1, step, 0, NY // 2)
        if not last:
            after[1].start()
            sums[0:3, :] = lax.fori_loop(0, 2, sample_one, jnp.zeros((3, 2 * M), F32))
            sample_outer(0)
        copies[2].wait()
        border(1, step, NY // 2, NY)
        spread_outer(1, step, NY // 2, NY)
        if last:
            part[step, 1, 0:3, :] = sample_planes(CZ - 1, other)
        else:
            sample_outer(1)
            part[step, 0, 0:3, :] = sums[0:3, own]
            part[step, 1, 0:3, :] = sums[0:3, other]
        answers = [
            pltpu.make_async_remote_copy(
                src_ref=part.at[step, k], dst_ref=got.at[step, k],
                send_sem=rsend.at[step, k], recv_sem=rrecv.at[step, k],
                device_id=(target,), device_id_type=MESH,
            )
            for k, target in ((1, left), (0, right))[: 1 if last else 2]
        ]
        for c in answers:
            c.start()
        if last:
            acc = sample_planes(CZ, own)
        else:
            after[2].start()
            copies = after
            interior(step + 1)
        for c in answers:
            c.wait_recv()
        if last:
            oout[...] = marks[0:3, own] + DT * (marks[7:8, own] * (acc + got[step, 1, 0:3, :]))
        else:
            marks[0:3, own] = marks[0:3, own] + DT * (
                marks[7:8, own] * (part[step, 0, 0:3, :] + got[step, 1, 0:3, :])
            )
            marks[0:3, other] = marks[0:3, other] + DT * (
                marks[7:8, other] * (got[step, 0, 0:3, :] + part[step, 1, 0:3, :])
            )
        waits += answers
    for c in waits:
        c.wait_send()


def local(velocity, offsets, bases, targets, stiffness, active_block_count):
    vmem = pl.BlockSpec(memory_space=pltpu.VMEM)
    hbm = pl.BlockSpec(memory_space=pltpu.HBM)
    return pl.pallas_call(
        kernel,
        out_shape=(
            jax.ShapeDtypeStruct(velocity.shape, F32),
            jax.ShapeDtypeStruct(offsets.shape, F32),
        ),
        in_specs=[hbm] * 6,
        out_specs=(vmem, vmem),
        scratch_shapes=[
            pltpu.VMEM((3, 2, LB, NY + 16, 128), F32),
            pltpu.VMEM((3, 2, LB, NY + 16, 128), F32),
            pltpu.VMEM((3, 2, LB, NY + 16, 128), F32),
            pltpu.VMEM((3, 2, LB, NY + 16, 128), F32),
            pltpu.VMEM((CZ, 3, NY, NX), BF),
            pltpu.VMEM((2, 3, NY, NX), BF),
            pltpu.VMEM((STEPS, 2, 3, NY, NX), BF),
            pltpu.VMEM((NX, 2 * M), BF),
            pltpu.VMEM((NY, 2 * M), F32),
            pltpu.VMEM((3 * NY, 2 * M), BF),
            pltpu.VMEM((CZ, 8, 2 * M), F32),
            pltpu.VMEM((CZ, 8, 2 * M), F32),
            pltpu.VMEM((8, 2 * M), F32),
            pltpu.VMEM((16, 2 * M), jnp.int32),
            pltpu.VMEM((16, 2 * M), F32),
            pltpu.VMEM((16, M), F32),
            pltpu.VMEM((16, M), F32),
            pltpu.VMEM((8, 2 * M), F32),
            pltpu.VMEM((STEPS, 2, 8, M), F32),
            pltpu.VMEM((STEPS, 2, 8, M), F32),
            pltpu.VMEM((3, M), F32),
            pltpu.VMEM((3, M), jnp.int32),
            pltpu.VMEM((3, M), F32),
            pltpu.VMEM((1, M), F32),
            pltpu.VMEM((1, 1), jnp.int32),
            pltpu.SemaphoreType.DMA((CZ, LB, 3)),
            pltpu.SemaphoreType.DMA((5,)),
            pltpu.SemaphoreType.DMA((STEPS, 3)),
            pltpu.SemaphoreType.DMA((STEPS, 3)),
            pltpu.SemaphoreType.DMA,
            pltpu.SemaphoreType.DMA,
            pltpu.SemaphoreType.DMA((STEPS, 2)),
            pltpu.SemaphoreType.DMA((STEPS, 2)),
        ],
        compiler_params=pltpu.CompilerParams(
            collective_id=0, has_side_effects=True, vmem_limit_bytes=40 * 1024 * 1024
        ),
    )(*(
        pltpu.with_memory_space_constraint(a, pltpu.HBM)
        for a in (
            velocity,
            offsets,
            bases,
            targets,
            stiffness.reshape(1, -1),
        )
    ), active_block_count.reshape(1, 1))


def solution(mesh):
    return jax.shard_map(
        local,
        mesh=mesh,
        in_specs=(
            P(None, AXIS, None, None),
            P(None, AXIS),
            P(None, AXIS),
            P(None, AXIS),
            P(AXIS),
            P(AXIS),
        ),
        out_specs=(P(None, AXIS, None, None), P(None, AXIS)),
        check_vma=False,
    )
```

```python
import math

import jax
import jax.numpy as jnp
from jax import lax
from jax.experimental import pallas as pl
from jax.experimental.pallas import tpu as pltpu
from jax.sharding import PartitionSpec as P

AXIS = "gz"
BLK = 256
STEPS = 2
DT = 0.2
NU = 0.3
CZ = 4
NY = 256
NX = 512
M = 512
LB = NX // 128
MESH = pl.DeviceIdType.MESH
BF = jnp.bfloat16
F32 = jnp.float32


def weights(offsets):
    angle = offsets * (0.5 * math.pi)
    c = 0.25 * jnp.cos(angle)
    s = 0.25 * jnp.sin(angle)
    return (0.25 + c, 0.25 + s, 0.25 - c, 0.25 - s)


def pick(delta, taps):
    out = jnp.where(delta == 3, taps[3], 0.0)
    for j in (2, 1, 0):
        out = jnp.where(delta == j, taps[j], out)
    return out


def kernel(
    vel, off_in, bases_in, targ_in, stiff_in, act_in,
    vout, oout,
    inner_a, outer_a, inner_b, outer_b, low, edge, halo, xtab, ytab, lhs, gains, zrows, taps, cells, marks, pack, near,
    sums, part, got, offs, bases_ref, targ_ref, stiff_ref, act_ref,
    in_sem, small_sem, send_sem, recv_sem, psend, precv, rsend, rrecv,
):
    me = lax.axis_index(AXIS)
    count = lax.axis_size(AXIS)
    right = lax.rem(me + 1, count)
    left = lax.rem(me + count - 1, count)

    core = lax.rem(me, 2)
    partner = (me + 1 - 2 * core, lax.rem(me + count - 1 + 2 * core, count))
    plane = (3 - 3 * core, 3 * core)
    at = (1 - core, core)
    smalls = [
        pltpu.make_async_copy(a, b, small_sem.at[i])
        for i, (a, b) in enumerate((
            (off_in, offs), (bases_in, bases_ref), (targ_in, targ_ref),
            (stiff_in, stiff_ref), (act_in, act_ref),
        ))
    ]
    for copy in smalls:
        copy.start()
    sets = ((inner_a, outer_a), (inner_b, outer_b))
    loads = {}
    for key, p, home, q in (
        ("slow", plane[1], outer_a, at[1]),
        ("fast", plane[0], outer_a, at[0]),
        (1, 1, inner_a, 0),
        (2, 2, inner_a, 1),
    ):
        number = len(loads)
        loads[key] = []
        for b in range(LB):
            lanes = pl.ds(b * 128, 128)
            for j, (rows, to) in enumerate((
                (pl.ds(0, NY), pl.ds(8, NY)),
                (pl.ds(NY - 8, 8), pl.ds(0, 8)),
                (pl.ds(0, 8), pl.ds(NY + 8, 8)),
            )):
                loads[key].append(pltpu.make_async_copy(
                    vel.at[:, p, rows, lanes], home.at[:, q, b, to, :], in_sem.at[number, b, j]
                ))
                loads[key][-1].start()

    barrier = pltpu.get_barrier_semaphore()
    for neighbour in (left, right):
        pl.semaphore_signal(barrier, inc=1, device_id=(neighbour,), device_id_type=MESH)

    for copy in smalls:
        copy.wait()
    lane = lax.broadcasted_iota(jnp.int32, (1, M), 1)
    living = jnp.where(lane < act_ref[...] * BLK, 1.0, 0.0)
    pack[0:3, :] = offs[...]
    pack[3:6, :] = targ_ref[...]
    pack[6:7, :] = living * stiff_ref[...]
    pack[7:8, :] = living
    pack[8:10, :] = bases_ref[0:2, :].astype(F32)
    pack[10:11, :] = (bases_ref[2:3, :] - me * CZ).astype(F32)
    pack[11:16, :] = jnp.zeros((5, M), F32)

    def prepare(half):
        o = marks[0:3, half]
        w = weights(o)
        force = marks[6:7, half] * (marks[3:6, half] - o)
        for j in range(4):
            taps[j : j + 1, half] = w[j][0:1]
            taps[4 + j : 5 + j, half] = w[j][1:2]
        for z in range(CZ):
            row = pick(z - cells[8:9, half], [w[j][2:3] for j in range(4)])
            zrows[z, 0:1, half] = row
            gains[z, 0:3, half] = force * row

    def tables(halves):
        def fill(table, extent, first, kind):
            def rows(i, _):
                r = pl.multiple_of(i * 32, 32)
                for half in halves:
                    where = lax.broadcasted_iota(jnp.int32, (32, M), 0) + r
                    out = 0.0
                    for j in range(4):
                        out = jnp.where(
                            where == cells[first + j : first + j + 1, half],
                            taps[first + j : first + j + 1, half],
                            out,
                        )
                    table[pl.ds(r, 32), half] = out.astype(kind)
                return 0

            lax.fori_loop(0, extent // 32, rows, 0)

        fill(xtab, NX, 0, BF)
        fill(ytab, NY, 4, F32)

    side = 1.0 - 2.0 * core.astype(F32)
    sides = (side, -side)
    lane128 = lax.broadcasted_iota(jnp.int32, (16, 128), 1)

    def stencil(src, dst, p, base, height, near_planes, sign=None):
        for h in range(height // 16):
            r = base + 16 * h
            turned = []
            for c in range(3):
                v = [src[c, p, b, pl.ds(r + 8, 16), :] for b in range(LB)]
                up = [pltpu.roll(x, 127, 1) for x in v]
                down = [pltpu.roll(x, 1, 1) for x in v]
                turned.append((
                    [jnp.where(lane128 == 127, up[(b + 1) % LB], up[b]) for b in range(LB)],
                    [jnp.where(lane128 == 0, down[(b - 1) % LB], down[b]) for b in range(LB)],
                ))
            for b in range(LB):
                v = [src[c, p, b, pl.ds(r + 8, 16), :] for c in range(3)]
                upper, lower = [], []
                for d in (2, 1, 0):
                    rate = 0.5 * DT if d != 2 or sign is None else 0.5 * DT * sign
                    scaled = rate * v[d]
                    upper.append(DT * NU - scaled)
                    lower.append(DT * NU + scaled)
                for c in range(3):
                    above, below = near_planes(c, b, r)
                    total = (1.0 - 6.0 * DT * NU) * v[c]
                    total = total + (upper[0] * above + lower[0] * below)
                    total = total + (
                        upper[1] * src[c, p, b, pl.ds(r + 9, 16), :]
                        + lower[1] * src[c, p, b, pl.ds(r + 7, 16), :]
                    )
                    total = total + (upper[2] * turned[c][0][b] + lower[2] * turned[c][1][b])
                    dst[c, p, b, pl.ds(r + 8, 16), :] = total

    def interior(step, which=(0, 1)):
        (inn, out), (dst, _) = sets[step], sets[1 - step]
        for q in which:

            def near_planes(c, b, r, q=q):
                middle = inn[c, 1 - q, b, pl.ds(r + 8, 16), :]
                edge_plane = out[c, q, b, pl.ds(r + 8, 16), :]
                return (edge_plane, middle) if q else (middle, edge_plane)

            def rows(i, _, q=q, near_planes=near_planes):
                stencil(inn, dst, q, pl.multiple_of(i * 128, 128), 128, near_planes)
                return 0

            lax.fori_loop(0, NY // 128, rows, 0)

    def border(slot, q, sign, step, start, stop):
        (inn, out), (_, dst) = sets[step], sets[1 - step]

        def near_planes(c, b, r):
            return (
                halo[step, slot, c, pl.ds(r, 16), b * 128 : b * 128 + 128].astype(F32),
                inn[c, q, b, pl.ds(r + 8, 16), :],
            )

        def rows(i, _):
            stencil(out, dst, q, pl.multiple_of(i * 128, 128), 128, near_planes, sign)
            return 0

        lax.fori_loop(start // 128, stop // 128, rows, 0)

    def spread(z, kind, q, step, start=0, stop=NY, width=2 * M):
        work = sets[1 - step][kind]
        height = stop - start
        for c in range(3):
            lhs[c * height : (c + 1) * height, 0:width] = (
                gains[z, c : c + 1, 0:width] * ytab[start:stop, 0:width]
            ).astype(BF)
        out = lax.dot_general(
            lhs[0 : 3 * height, 0:width],
            xtab[:, 0:width],
            (((1,), (1,)), ((), ())),
            preferred_element_type=F32,
        ).reshape(3, height, NX)
        for b in range(LB):
            lanes = slice(b * 128, b * 128 + 128)
            total = work[:, q, b, start + 8 : stop + 8, :] + DT * out[:, :, lanes]
            if step + 1 < STEPS:
                work[:, q, b, start + 8 : stop + 8, :] = total
                if stop == NY:
                    work[:, q, b, 0:8, :] = total[:, height - 8 :]
                if start == 0:
                    work[:, q, b, NY + 8 :, :] = total[:, :8]
            else:
                vout[:, z, start:stop, lanes] = total
            low[z, :, start:stop, lanes] = total.astype(BF)

    own, other = slice(0, M), slice(M, 2 * M)
    both = slice(0, 2 * M)

    def reduce_rows(out, z, half):
        y = ytab[:, half]
        parts = [jnp.sum(out[c * NY : (c + 1) * NY] * y, axis=0, keepdims=True) for c in range(3)]
        return jnp.concatenate(parts, axis=0) * zrows[z, 0:1, half]

    def sample(z, half=both):
        out = jnp.dot(low[z].reshape(3 * NY, NX), xtab[:, half], preferred_element_type=F32)
        return reduce_rows(out, z, half)

    def spread_outer(k, step, start, stop):
        @pl.when(core == k)
        def _():
            spread(CZ - 1, 1, 1, step, start, stop, M)

        @pl.when(core != k)
        def _():
            spread(0, 1, 0, step, start, stop)

    def sample_outer(k):
        @pl.when(core == k)
        def _():
            sums[0:3, own] = sums[0:3, own] + sample(CZ - 1, own)

        @pl.when(core != k)
        def _():
            sums[0:3, :] = sums[0:3, :] + sample(0)

    def sample_planes(planes, half):
        out = jnp.dot(
            low[0:planes].reshape(planes * 3 * NY, NX), xtab[:, half], preferred_element_type=F32
        )
        total = 0.0
        for z in range(planes):
            total = total + reduce_rows(out[z * 3 * NY : (z + 1) * 3 * NY], z, half)
        return total

    pieces = ((0, 0, NY), (1, 0, NY // 2), (1, NY // 2, NY))

    def sending(step, ref_of):
        out = []
        for i, (k, start, stop) in enumerate(pieces):
            rows = pl.ds(start, stop - start)
            out.append(pltpu.make_async_remote_copy(
                src_ref=ref_of(k).at[:, rows, :], dst_ref=halo.at[step, k, :, rows, :],
                send_sem=send_sem.at[step, i], recv_sem=recv_sem.at[step, i],
                device_id=(partner[k],), device_id_type=MESH,
            ))
        return out

    packet = pltpu.make_async_remote_copy(
        src_ref=pack, dst_ref=near, send_sem=psend, recv_sem=precv,
        device_id=(right,), device_id_type=MESH,
    )
    copies = sending(0, lambda k: edge.at[k])

    def lower_edge(k):
        def rows(i, _):
            r = pl.multiple_of(i * 16, 16)
            for c in range(3):
                for b in range(LB):
                    edge[k, c, pl.ds(r, 16), b * 128 : b * 128 + 128] = (
                        outer_a[c, at[k], b, pl.ds(r + 8, 16), :].astype(BF)
                    )
            return 0

        lax.fori_loop(0, NY // 16, rows, 0)

    def columns(half, shift):
        for j in range(4):
            cells[j : j + 1, half] = (marks[8:9, half].astype(jnp.int32) + j) & (NX - 1)
            cells[4 + j : 5 + j, half] = (marks[9:10, half].astype(jnp.int32) + j) & (NY - 1)
        cells[8:9, half] = marks[10:11, half].astype(jnp.int32) - shift

    for c in loads["slow"]:
        c.wait()
    lower_edge(1)
    pl.semaphore_wait(barrier, 2)
    packet.start()
    copies[1].start()
    copies[2].start()
    for c in loads["fast"]:
        c.wait()
    lower_edge(0)
    copies[0].start()
    marks[:, own] = pack[...]
    columns(own, 0)
    prepare(own)
    tables((own,))
    for c in loads[1] + loads[2]:
        c.wait()
    interior(0)
    def outer_border(k, step, start, stop):
        border(k, at[k], sides[k], step, start, stop)

    copies[0].wait()
    outer_border(0, 0, 0, NY)
    packet.wait_recv()
    marks[:, other] = near[...]
    columns(other, CZ)
    prepare(other)
    tables((other,))

    spread(1, 0, 0, 0)
    spread(2, 0, 1, 0)
    spread_outer(0, 0, 0, NY)
    after = sending(1, lambda k: low.at[plane[k]])
    after[0].start()
    copies[1].wait()
    outer_border(1, 0, 0, NY // 2)
    spread_outer(1, 0, 0, NY // 2)
    after[1].start()
    sums[0:3, :] = sample(1) + sample(2)
    sample_outer(0)
    copies[2].wait()
    outer_border(1, 0, NY // 2, NY)
    spread_outer(1, 0, NY // 2, NY)
    sample_outer(1)
    part[0, 0, 0:3, :] = sums[0:3, own]
    part[0, 1, 0:3, :] = sums[0:3, other]

    def exchange(step, k, target):
        return pltpu.make_async_remote_copy(
            src_ref=part.at[step, k], dst_ref=got.at[step, k],
            send_sem=rsend.at[step, k], recv_sem=rrecv.at[step, k],
            device_id=(target,), device_id_type=MESH,
        )

    answers = [exchange(0, 0, right), exchange(0, 1, left)]
    for c in answers:
        c.start()
    after[2].start()
    interior(1)
    after[0].wait()
    outer_border(0, 1, 0, NY)
    for c in answers:
        c.wait_recv()
    marks[0:3, own] = marks[0:3, own] + DT * (
        marks[7:8, own] * (part[0, 0, 0:3, :] + got[0, 1, 0:3, :])
    )
    marks[0:3, other] = marks[0:3, other] + DT * (
        marks[7:8, other] * (got[0, 0, 0:3, :] + part[0, 1, 0:3, :])
    )
    prepare(both)
    tables((own, other))
    spread(1, 0, 0, 1)
    spread(2, 0, 1, 1)
    for c in after[1:]:
        c.wait()
    outer_border(1, 1, 0, NY)
    spread(0, 1, 0, 1)
    part[1, 1, 0:3, :] = sample_planes(CZ - 1, other)
    answer = exchange(1, 1, left)
    answer.start()
    spread(CZ - 1, 1, 1, 1, 0, NY, M)
    acc = sample_planes(CZ, own)
    answer.wait_recv()
    oout[...] = marks[0:3, own] + DT * (marks[7:8, own] * (acc + got[1, 1, 0:3, :]))
    for c in [packet, answer] + answers:
        c.wait_send()


def local(velocity, offsets, bases, targets, stiffness, active_block_count):
    vmem = pl.BlockSpec(memory_space=pltpu.VMEM)
    hbm = pl.BlockSpec(memory_space=pltpu.HBM)
    return pl.pallas_call(
        kernel,
        out_shape=(
            jax.ShapeDtypeStruct(velocity.shape, F32),
            jax.ShapeDtypeStruct(offsets.shape, F32),
        ),
        in_specs=[hbm] * 6,
        out_specs=(vmem, vmem),
        scratch_shapes=[
            pltpu.VMEM((3, 2, LB, NY + 16, 128), F32),
            pltpu.VMEM((3, 2, LB, NY + 16, 128), F32),
            pltpu.VMEM((3, 2, LB, NY + 16, 128), F32),
            pltpu.VMEM((3, 2, LB, NY + 16, 128), F32),
            pltpu.VMEM((CZ, 3, NY, NX), BF),
            pltpu.VMEM((2, 3, NY, NX), BF),
            pltpu.VMEM((STEPS, 2, 3, NY, NX), BF),
            pltpu.VMEM((NX, 2 * M), BF),
            pltpu.VMEM((NY, 2 * M), F32),
            pltpu.VMEM((3 * NY, 2 * M), BF),
            pltpu.VMEM((CZ, 8, 2 * M), F32),
            pltpu.VMEM((CZ, 8, 2 * M), F32),
            pltpu.VMEM((8, 2 * M), F32),
            pltpu.VMEM((16, 2 * M), jnp.int32),
            pltpu.VMEM((16, 2 * M), F32),
            pltpu.VMEM((16, M), F32),
            pltpu.VMEM((16, M), F32),
            pltpu.VMEM((8, 2 * M), F32),
            pltpu.VMEM((STEPS, 2, 8, M), F32),
            pltpu.VMEM((STEPS, 2, 8, M), F32),
            pltpu.VMEM((3, M), F32),
            pltpu.VMEM((3, M), jnp.int32),
            pltpu.VMEM((3, M), F32),
            pltpu.VMEM((1, M), F32),
            pltpu.VMEM((1, 1), jnp.int32),
            pltpu.SemaphoreType.DMA((CZ, LB, 3)),
            pltpu.SemaphoreType.DMA((5,)),
            pltpu.SemaphoreType.DMA((STEPS, 3)),
            pltpu.SemaphoreType.DMA((STEPS, 3)),
            pltpu.SemaphoreType.DMA,
            pltpu.SemaphoreType.DMA,
            pltpu.SemaphoreType.DMA((STEPS, 2)),
            pltpu.SemaphoreType.DMA((STEPS, 2)),
        ],
        compiler_params=pltpu.CompilerParams(
            collective_id=0, has_side_effects=True, vmem_limit_bytes=40 * 1024 * 1024
        ),
    )(*(
        pltpu.with_memory_space_constraint(a, pltpu.HBM)
        for a in (
            velocity,
            offsets,
            bases,
            targets,
            stiffness.reshape(1, -1),
        )
    ), active_block_count.reshape(1, 1))


def solution(mesh):
    return jax.shard_map(
        local,
        mesh=mesh,
        in_specs=(
            P(None, AXIS, None, None),
            P(None, AXIS),
            P(None, AXIS),
            P(None, AXIS),
            P(AXIS),
            P(AXIS),
        ),
        out_specs=(P(None, AXIS, None, None), P(None, AXIS)),
        check_vma=False,
    )
```

```python
import math

import jax
import jax.numpy as jnp
from jax import lax
from jax.experimental import pallas as pl
from jax.experimental.pallas import tpu as pltpu
from jax.sharding import PartitionSpec as P

AXIS = "gz"
BLK = 256
STEPS = 2
DT = 0.2
NU = 0.3
CZ = 4
NY = 256
NX = 512
M = 512
LB = NX // 128
MESH = pl.DeviceIdType.MESH
BF = jnp.bfloat16
F32 = jnp.float32


def weights(offsets):
    angle = offsets * (0.5 * math.pi)
    c = 0.25 * jnp.cos(angle)
    s = 0.25 * jnp.sin(angle)
    return (0.25 + c, 0.25 + s, 0.25 - c, 0.25 - s)


def pick(delta, taps):
    out = jnp.where(delta == 3, taps[3], 0.0)
    for j in (2, 1, 0):
        out = jnp.where(delta == j, taps[j], out)
    return out


def kernel(
    vel, off_in, bases_in, targ_in, stiff_in, act_in,
    vout, oout,
    inner_a, outer_a, inner_b, outer_b, low, edge, halo, xtab, ytab, lhs, gains, zrows, taps, cells, marks, pack, near,
    sums, part, got, offs, bases_ref, targ_ref, stiff_ref, act_ref,
    in_sem, small_sem, send_sem, recv_sem, psend, precv, rsend, rrecv,
):
    me = lax.axis_index(AXIS)
    count = lax.axis_size(AXIS)
    right = lax.rem(me + 1, count)
    left = lax.rem(me + count - 1, count)

    core = lax.rem(me, 2)
    partner = (me + 1 - 2 * core, lax.rem(me + count - 1 + 2 * core, count))
    plane = (3 - 3 * core, 3 * core)
    at = (1 - core, core)
    smalls = [
        pltpu.make_async_copy(a, b, small_sem.at[i])
        for i, (a, b) in enumerate((
            (off_in, offs), (bases_in, bases_ref), (targ_in, targ_ref),
            (stiff_in, stiff_ref), (act_in, act_ref),
        ))
    ]
    for copy in smalls:
        copy.start()
    sets = ((inner_a, outer_a), (inner_b, outer_b))
    loads = {}
    for key, p, home, q in (
        ("slow", plane[1], outer_a, at[1]),
        ("fast", plane[0], outer_a, at[0]),
        (1, 1, inner_a, 0),
        (2, 2, inner_a, 1),
    ):
        number = len(loads)
        loads[key] = []
        for b in range(LB):
            lanes = pl.ds(b * 128, 128)
            for j, (rows, to) in enumerate((
                (pl.ds(0, NY), pl.ds(8, NY)),
                (pl.ds(NY - 8, 8), pl.ds(0, 8)),
                (pl.ds(0, 8), pl.ds(NY + 8, 8)),
            )):
                loads[key].append(pltpu.make_async_copy(
                    vel.at[:, p, rows, lanes], home.at[:, q, b, to, :], in_sem.at[number, b, j]
                ))
                loads[key][-1].start()

    barrier = pltpu.get_barrier_semaphore()
    for neighbour in (left, right):
        pl.semaphore_signal(barrier, inc=1, device_id=(neighbour,), device_id_type=MESH)

    for copy in smalls:
        copy.wait()
    lane = lax.broadcasted_iota(jnp.int32, (1, M), 1)
    living = jnp.where(lane < act_ref[...] * BLK, 1.0, 0.0)
    pack[0:3, :] = offs[...]
    pack[3:6, :] = targ_ref[...]
    pack[6:7, :] = living * stiff_ref[...]
    pack[7:8, :] = living
    pack[8:10, :] = bases_ref[0:2, :].astype(F32)
    pack[10:11, :] = (bases_ref[2:3, :] - me * CZ).astype(F32)
    pack[11:16, :] = jnp.zeros((5, M), F32)

    def prepare(half):
        o = marks[0:3, half]
        w = weights(o)
        force = marks[6:7, half] * (marks[3:6, half] - o)
        for j in range(4):
            taps[j : j + 1, half] = w[j][0:1]
            taps[4 + j : 5 + j, half] = w[j][1:2]
        for z in range(CZ):
            row = pick(z - cells[8:9, half], [w[j][2:3] for j in range(4)])
            zrows[z, 0:1, half] = row
            gains[z, 0:3, half] = force * row

    def tables(halves):
        def fill(table, extent, first, kind):
            def rows(i, _):
                r = pl.multiple_of(i * 32, 32)
                for half in halves:
                    where = lax.broadcasted_iota(jnp.int32, (32, M), 0) + r
                    out = 0.0
                    for j in range(4):
                        out = jnp.where(
                            where == cells[first + j : first + j + 1, half],
                            taps[first + j : first + j + 1, half],
                            out,
                        )
                    table[pl.ds(r, 32), half] = out.astype(kind)
                return 0

            lax.fori_loop(0, extent // 32, rows, 0)

        fill(xtab, NX, 0, BF)
        fill(ytab, NY, 4, F32)

    side = 1.0 - 2.0 * core.astype(F32)
    sides = (side, -side)
    lane128 = lax.broadcasted_iota(jnp.int32, (16, 128), 1)

    def stencil(src, dst, p, base, height, near_planes, sign=None):
        for h in range(height // 16):
            r = base + 16 * h
            turned = []
            for c in range(3):
                v = [src[c, p, b, pl.ds(r + 8, 16), :] for b in range(LB)]
                up = [pltpu.roll(x, 127, 1) for x in v]
                down = [pltpu.roll(x, 1, 1) for x in v]
                turned.append((
                    [jnp.where(lane128 == 127, up[(b + 1) % LB], up[b]) for b in range(LB)],
                    [jnp.where(lane128 == 0, down[(b - 1) % LB], down[b]) for b in range(LB)],
                ))
            for b in range(LB):
                v = [src[c, p, b, pl.ds(r + 8, 16), :] for c in range(3)]
                upper, lower = [], []
                for d in (2, 1, 0):
                    rate = 0.5 * DT if d != 2 or sign is None else 0.5 * DT * sign
                    scaled = rate * v[d]
                    upper.append(DT * NU - scaled)
                    lower.append(DT * NU + scaled)
                for c in range(3):
                    above, below = near_planes(c, b, r)
                    total = (1.0 - 6.0 * DT * NU) * v[c]
                    total = total + (upper[0] * above + lower[0] * below)
                    total = total + (
                        upper[1] * src[c, p, b, pl.ds(r + 9, 16), :]
                        + lower[1] * src[c, p, b, pl.ds(r + 7, 16), :]
                    )
                    total = total + (upper[2] * turned[c][0][b] + lower[2] * turned[c][1][b])
                    dst[c, p, b, pl.ds(r + 8, 16), :] = total

    def interior(step, which=(0, 1)):
        (inn, out), (dst, _) = sets[step], sets[1 - step]
        for q in which:

            def near_planes(c, b, r, q=q):
                middle = inn[c, 1 - q, b, pl.ds(r + 8, 16), :]
                edge_plane = out[c, q, b, pl.ds(r + 8, 16), :]
                return (edge_plane, middle) if q else (middle, edge_plane)

            def rows(i, _, q=q, near_planes=near_planes):
                stencil(inn, dst, q, pl.multiple_of(i * 256, 256), 256, near_planes)
                return 0

            lax.fori_loop(0, NY // 256, rows, 0)

    def border(slot, q, sign, step, start, stop):
        (inn, out), (_, dst) = sets[step], sets[1 - step]

        def near_planes(c, b, r):
            return (
                halo[step, slot, c, pl.ds(r, 16), b * 128 : b * 128 + 128].astype(F32),
                inn[c, q, b, pl.ds(r + 8, 16), :],
            )

        def rows(i, _):
            stencil(out, dst, q, pl.multiple_of(i * 128, 128), 128, near_planes, sign)
            return 0

        lax.fori_loop(start // 128, stop // 128, rows, 0)

    def spread(z, kind, q, step, start=0, stop=NY, width=2 * M):
        work = sets[1 - step][kind]
        height = stop - start
        for c in range(3):
            lhs[c * height : (c + 1) * height, 0:width] = (
                gains[z, c : c + 1, 0:width] * ytab[start:stop, 0:width]
            ).astype(BF)
        out = lax.dot_general(
            lhs[0 : 3 * height, 0:width],
            xtab[:, 0:width],
            (((1,), (1,)), ((), ())),
            preferred_element_type=F32,
        ).reshape(3, height, NX)
        for b in range(LB):
            lanes = slice(b * 128, b * 128 + 128)
            total = work[:, q, b, start + 8 : stop + 8, :] + DT * out[:, :, lanes]
            if step + 1 < STEPS:
                work[:, q, b, start + 8 : stop + 8, :] = total
                if stop == NY:
                    work[:, q, b, 0:8, :] = total[:, height - 8 :]
                if start == 0:
                    work[:, q, b, NY + 8 :, :] = total[:, :8]
            else:
                vout[:, z, start:stop, lanes] = total
            low[z, :, start:stop, lanes] = total.astype(BF)

    own, other = slice(0, M), slice(M, 2 * M)
    both = slice(0, 2 * M)

    def reduce_rows(out, z, half):
        y = ytab[:, half]
        parts = [jnp.sum(out[c * NY : (c + 1) * NY] * y, axis=0, keepdims=True) for c in range(3)]
        return jnp.concatenate(parts, axis=0) * zrows[z, 0:1, half]

    def sample(z, half=both):
        out = jnp.dot(low[z].reshape(3 * NY, NX), xtab[:, half], preferred_element_type=F32)
        return reduce_rows(out, z, half)

    def spread_outer(k, step, start, stop):
        @pl.when(core == k)
        def _():
            spread(CZ - 1, 1, 1, step, start, stop, M)

        @pl.when(core != k)
        def _():
            spread(0, 1, 0, step, start, stop)

    def sample_outer(k):
        @pl.when(core == k)
        def _():
            sums[0:3, own] = sums[0:3, own] + sample(CZ - 1, own)

        @pl.when(core != k)
        def _():
            sums[0:3, :] = sums[0:3, :] + sample(0)

    def sample_planes(planes, half):
        out = jnp.dot(
            low[0:planes].reshape(planes * 3 * NY, NX), xtab[:, half], preferred_element_type=F32
        )
        total = 0.0
        for z in range(planes):
            total = total + reduce_rows(out[z * 3 * NY : (z + 1) * 3 * NY], z, half)
        return total

    pieces = ((0, 0, NY), (1, 0, NY // 2), (1, NY // 2, NY))

    def sending(step, ref_of):
        out = []
        for i, (k, start, stop) in enumerate(pieces):
            rows = pl.ds(start, stop - start)
            out.append(pltpu.make_async_remote_copy(
                src_ref=ref_of(k).at[:, rows, :], dst_ref=halo.at[step, k, :, rows, :],
                send_sem=send_sem.at[step, i], recv_sem=recv_sem.at[step, i],
                device_id=(partner[k],), device_id_type=MESH,
            ))
        return out

    packet = pltpu.make_async_remote_copy(
        src_ref=pack, dst_ref=near, send_sem=psend, recv_sem=precv,
        device_id=(right,), device_id_type=MESH,
    )
    copies = sending(0, lambda k: edge.at[k])

    def lower_edge(k):
        def rows(i, _):
            r = pl.multiple_of(i * 16, 16)
            for c in range(3):
                for b in range(LB):
                    edge[k, c, pl.ds(r, 16), b * 128 : b * 128 + 128] = (
                        outer_a[c, at[k], b, pl.ds(r + 8, 16), :].astype(BF)
                    )
            return 0

        lax.fori_loop(0, NY // 16, rows, 0)

    def columns(half, shift):
        for j in range(4):
            cells[j : j + 1, half] = (marks[8:9, half].astype(jnp.int32) + j) & (NX - 1)
            cells[4 + j : 5 + j, half] = (marks[9:10, half].astype(jnp.int32) + j) & (NY - 1)
        cells[8:9, half] = marks[10:11, half].astype(jnp.int32) - shift

    for c in loads["slow"]:
        c.wait()
    lower_edge(1)
    pl.semaphore_wait(barrier, 2)
    packet.start()
    copies[1].start()
    copies[2].start()
    for c in loads["fast"]:
        c.wait()
    lower_edge(0)
    copies[0].start()
    marks[:, own] = pack[...]
    columns(own, 0)
    prepare(own)
    tables((own,))
    for c in loads[1] + loads[2]:
        c.wait()
    interior(0)
    def outer_border(k, step, start, stop):
        border(k, at[k], sides[k], step, start, stop)

    copies[0].wait()
    outer_border(0, 0, 0, NY)
    packet.wait_recv()
    marks[:, other] = near[...]
    columns(other, CZ)
    prepare(other)
    tables((other,))

    spread(1, 0, 0, 0)
    spread(2, 0, 1, 0)
    spread_outer(0, 0, 0, NY)
    after = sending(1, lambda k: low.at[plane[k]])
    after[0].start()
    copies[1].wait()
    outer_border(1, 0, 0, NY // 2)
    spread_outer(1, 0, 0, NY // 2)
    after[1].start()
    sums[0:3, :] = sample(1) + sample(2)
    sample_outer(0)
    copies[2].wait()
    outer_border(1, 0, NY // 2, NY)
    spread_outer(1, 0, NY // 2, NY)
    sample_outer(1)
    part[0, 0, 0:3, :] = sums[0:3, own]
    part[0, 1, 0:3, :] = sums[0:3, other]

    def exchange(step, k, target):
        return pltpu.make_async_remote_copy(
            src_ref=part.at[step, k], dst_ref=got.at[step, k],
            send_sem=rsend.at[step, k], recv_sem=rrecv.at[step, k],
            device_id=(target,), device_id_type=MESH,
        )

    answers = [exchange(0, 0, right), exchange(0, 1, left)]
    for c in answers:
        c.start()
    after[2].start()
    interior(1)
    after[0].wait()
    outer_border(0, 1, 0, NY)
    for c in answers:
        c.wait_recv()
    marks[0:3, own] = marks[0:3, own] + DT * (
        marks[7:8, own] * (part[0, 0, 0:3, :] + got[0, 1, 0:3, :])
    )
    marks[0:3, other] = marks[0:3, other] + DT * (
        marks[7:8, other] * (got[0, 0, 0:3, :] + part[0, 1, 0:3, :])
    )
    prepare(both)
    tables((own, other))
    spread(1, 0, 0, 1)
    spread(2, 0, 1, 1)
    for c in after[1:]:
        c.wait()
    outer_border(1, 1, 0, NY)
    spread(0, 1, 0, 1)
    part[1, 1, 0:3, :] = sample_planes(CZ - 1, other)
    answer = exchange(1, 1, left)
    answer.start()
    spread(CZ - 1, 1, 1, 1, 0, NY, M)
    acc = sample_planes(CZ, own)
    answer.wait_recv()
    oout[...] = marks[0:3, own] + DT * (marks[7:8, own] * (acc + got[1, 1, 0:3, :]))
    for c in [packet, answer] + answers:
        c.wait_send()


def local(velocity, offsets, bases, targets, stiffness, active_block_count):
    vmem = pl.BlockSpec(memory_space=pltpu.VMEM)
    hbm = pl.BlockSpec(memory_space=pltpu.HBM)
    return pl.pallas_call(
        kernel,
        out_shape=(
            jax.ShapeDtypeStruct(velocity.shape, F32),
            jax.ShapeDtypeStruct(offsets.shape, F32),
        ),
        in_specs=[hbm] * 6,
        out_specs=(vmem, vmem),
        scratch_shapes=[
            pltpu.VMEM((3, 2, LB, NY + 16, 128), F32),
            pltpu.VMEM((3, 2, LB, NY + 16, 128), F32),
            pltpu.VMEM((3, 2, LB, NY + 16, 128), F32),
            pltpu.VMEM((3, 2, LB, NY + 16, 128), F32),
            pltpu.VMEM((CZ, 3, NY, NX), BF),
            pltpu.VMEM((2, 3, NY, NX), BF),
            pltpu.VMEM((STEPS, 2, 3, NY, NX), BF),
            pltpu.VMEM((NX, 2 * M), BF),
            pltpu.VMEM((NY, 2 * M), F32),
            pltpu.VMEM((3 * NY, 2 * M), BF),
            pltpu.VMEM((CZ, 8, 2 * M), F32),
            pltpu.VMEM((CZ, 8, 2 * M), F32),
            pltpu.VMEM((8, 2 * M), F32),
            pltpu.VMEM((16, 2 * M), jnp.int32),
            pltpu.VMEM((16, 2 * M), F32),
            pltpu.VMEM((16, M), F32),
            pltpu.VMEM((16, M), F32),
            pltpu.VMEM((8, 2 * M), F32),
            pltpu.VMEM((STEPS, 2, 8, M), F32),
            pltpu.VMEM((STEPS, 2, 8, M), F32),
            pltpu.VMEM((3, M), F32),
            pltpu.VMEM((3, M), jnp.int32),
            pltpu.VMEM((3, M), F32),
            pltpu.VMEM((1, M), F32),
            pltpu.VMEM((1, 1), jnp.int32),
            pltpu.SemaphoreType.DMA((CZ, LB, 3)),
            pltpu.SemaphoreType.DMA((5,)),
            pltpu.SemaphoreType.DMA((STEPS, 3)),
            pltpu.SemaphoreType.DMA((STEPS, 3)),
            pltpu.SemaphoreType.DMA,
            pltpu.SemaphoreType.DMA,
            pltpu.SemaphoreType.DMA((STEPS, 2)),
            pltpu.SemaphoreType.DMA((STEPS, 2)),
        ],
        compiler_params=pltpu.CompilerParams(
            collective_id=0, has_side_effects=True, vmem_limit_bytes=40 * 1024 * 1024
        ),
    )(*(
        pltpu.with_memory_space_constraint(a, pltpu.HBM)
        for a in (
            velocity,
            offsets,
            bases,
            targets,
            stiffness.reshape(1, -1),
        )
    ), active_block_count.reshape(1, 1))


def solution(mesh):
    return jax.shard_map(
        local,
        mesh=mesh,
        in_specs=(
            P(None, AXIS, None, None),
            P(None, AXIS),
            P(None, AXIS),
            P(None, AXIS),
            P(AXIS),
            P(AXIS),
        ),
        out_specs=(P(None, AXIS, None, None), P(None, AXIS)),
        check_vma=False,
    )
```
